32 devices in a mesh: section: 2 (over x), seq: 8 (over z, y), rep: 2 (over core).
Axes of the slice: x: 2, y: 2, z: 4, core: 2. Of those that a mesh axis runs over, the one named last changes fastest.
Arguments:
- queries: bfloat16 [512, 2560], P('seq', ('section', 'rep')), may hold values from -5 to 5
- keys: bfloat16 [512, 2560], P('seq', ('section', 'rep')), may hold values from -5 to 5
- values: bfloat16 [512, 2560], P('seq', ('section', 'rep')), may hold values from -6 to 6
- block_order: int32 [16], replicated, may hold values from 0 to 15, each once
- wo: bfloat16 [2560, 5120], P(('section', 'rep'), 'seq'), may hold values from -0.125 to 0.125
- resid: bfloat16 [4, 5120, 128], P(('section', 'rep'), 'seq'), may hold values from -60 to 60
- gain: bfloat16 [5120], P('seq'), may hold values from 0.099609375 to 1.8984375
- w_gate: bfloat16 [13824, 5120], P('seq'), may hold values from -0.078125 to 0.078125
- w_up: bfloat16 [13824, 5120], P('seq'), may hold values from -0.078125 to 0.078125
- w_down: bfloat16 [13824, 5120], P('seq'), may hold values from -0.0625 to 0.0625
Outputs:
- mixed: bfloat16 [4, 5120, 128], P(('section', 'rep'), 'seq')
The draws below stay inside these ranges and needn't reach their ends.
Inputs may be any that keep to these rules, and one draw needn't show every extreme that they name: `block_order`: each number once.
All inputs are finite; a program needn't handle non-finite values.
Results may differ from the reference program's by a relative error of at most 0.0055.
Values may be sent and summed in bfloat16 or wider, within the bound.
A program may use at most 128 MiB of HBM per device.

```python
import jax
import jax.numpy as jnp
from jax import lax

D = 5120
FF = 13824
HEADS = 20
HEAD_DIM = 128
SEQ_DEV = 64
TOKENS = 512
HW = 2560
GROUPS = 4
SUB = 16
BLOCKS = 16
N_SEQ = 8


def query_key_pair(key):
    queries = jnp.clip(jax.random.normal(jax.random.fold_in(key, 11), (TOKENS, HW), jnp.float32), -5.0, 5.0)
    keys = jnp.clip(jax.random.normal(jax.random.fold_in(key, 12), (TOKENS, HW), jnp.float32), -5.0, 5.0)
    return (queries, keys)


def draw_queries(key, part):
    return query_key_pair(key)[0].astype(jnp.bfloat16)


def draw_keys(key, part):
    return query_key_pair(key)[1].astype(jnp.bfloat16)


def draw_resid(key, part):
    base = jnp.clip(jax.random.normal(jax.random.fold_in(key, 21), (GROUPS, D, N_SEQ * SUB), jnp.float32), -6.0, 6.0)
    rising = (3.0 ** (jnp.arange(D, dtype=jnp.float32) / D)).reshape(1, D, 1)
    return jnp.clip(base * rising, -60.0, 60.0).astype(jnp.bfloat16)


def raised(entries, rng, source, target, blocks, factor):
    def block_of(axis_at):
        return (jnp.arange(entries.shape[axis_at]) // (entries.shape[axis_at] // blocks)).reshape((-1,) + (1,) * (entries.ndim - 1 - axis_at))

    one_side = jax.random.permutation(rng, blocks)[block_of(target)]
    second = (block_of(target) + blocks // 2) % blocks
    return jnp.where((block_of(source) == one_side) | (block_of(source) == second), factor * entries, entries)


def shard_levels(stream_key, dims, pieces, least, top_value):
    loudness = 1.0
    for position, parts in pieces:
        draws = jax.random.uniform(jax.random.fold_in(jax.random.fold_in(stream_key, 6), position), (parts,), jnp.float32, least / len(pieces), top_value / len(pieces))
        loudness = loudness * jnp.repeat(jnp.exp(draws), dims[position] // parts).reshape((-1,) + (1,) * (len(dims) - 1 - position))
    return loudness


def gaussian(rng, dims, spread, bound, shards=(), held_as=jnp.bfloat16):
    level = shard_levels(rng, dims, shards, -0.22, 0.18) if shards else 1.0
    result = jax.random.normal(rng, dims, jnp.float32) * spread * level
    return jnp.minimum(jnp.maximum(result, -bound), bound).astype(held_as)


def heavy_noise(own_key, shape, scale, limit, pieces, heavy, kind=jnp.bfloat16):
    values = scale * jax.random.normal(own_key, shape, jnp.float32)
    if pieces:
        values = values * shard_levels(own_key, shape, pieces, -0.22, 0.18)
    return jnp.clip(raised(values, jax.random.fold_in(own_key, 3), *heavy), -limit, limit).astype(kind)


def setup_inputs(seed: int = 0) -> dict:
    key_of = jax.random.split(jax.random.key(seed), 11)
    return {
        "queries": draw_queries(jax.random.fold_in(key_of[10], 71), 0),
        "keys": draw_keys(jax.random.fold_in(key_of[10], 71), 0),
        "values": gaussian(key_of[2], (TOKENS, HW), 1.0, 6.0, ((0, 8), (1, 4))),
        "block_order": jax.random.permutation(key_of[3], BLOCKS).astype(jnp.int32),
        "wo": gaussian(key_of[4], (HW, D), HW ** -0.5, 0.125, ((0, 4), (1, 8))),
        "resid": draw_resid(jax.random.fold_in(key_of[10], 71), 0),
        "gain": jnp.clip(1.0 + 0.18 * jax.random.normal(key_of[6], (D,), jnp.float32), 0.099609375, 1.8984375).astype(jnp.bfloat16),
        "w_gate": gaussian(key_of[7], (FF, D), D ** -0.5, 0.078125, ((0, 8),)),
        "w_up": gaussian(key_of[8], (FF, D), D ** -0.5, 0.078125, ((0, 8),)),
        "w_down": heavy_noise(key_of[9], (FF, D), FF ** -0.5, 0.0625, ((0, 8),), (0, 1, 8, 2.0)),
    }


def reference(queries, keys, values, block_order, wo, resid, gain, w_gate, w_up, w_down):
    block_rows = SEQ_DEV // 2
    row_ids = jnp.arange(TOKENS, dtype=jnp.int32)
    pos = block_order[row_ids // block_rows].astype(jnp.int32) * block_rows + row_ids % block_rows
    visible = pos[None, :] <= pos[:, None]
    scale = HEAD_DIM ** (-0.5)
    query_heads = queries.reshape(TOKENS, HEADS, HEAD_DIM).transpose(1, 0, 2)
    key_heads = keys.reshape(TOKENS, HEADS, HEAD_DIM).transpose(1, 0, 2)
    value_heads = values.reshape(TOKENS, HEADS, HEAD_DIM).transpose(1, 0, 2)

    def one_head(operands):
        q_head, k_head, v_head = operands
        scores = jnp.dot(q_head, k_head.T, preferred_element_type=jnp.float32) * scale
        scores = jnp.where(visible, scores, -jnp.inf)
        top = lax.optimization_barrier(jnp.max(scores, axis=-1, keepdims=True))
        probs = jnp.exp(scores - top)
        total = lax.optimization_barrier(jnp.sum(probs, axis=-1, keepdims=True))
        out = jnp.dot(probs.astype(jnp.bfloat16), v_head, preferred_element_type=jnp.float32) / total
        return out.astype(jnp.bfloat16)
    attended = lax.map(one_head, (query_heads, key_heads, value_heads))
    attended = attended.transpose(1, 0, 2).reshape(TOKENS, HW)
    resid_rows = resid.reshape(GROUPS, D, N_SEQ, SUB).transpose(2, 0, 3, 1).reshape(TOKENS, D)
    carried = resid_rows.astype(jnp.float32) + jnp.dot(attended, wo, preferred_element_type=jnp.float32)
    meansq = lax.optimization_barrier(jnp.mean(carried * carried, axis=-1, keepdims=True))
    normed = (carried * lax.rsqrt(meansq + 1e-05) * gain.astype(jnp.float32)).astype(jnp.bfloat16)
    gate = jnp.dot(normed, w_gate.T, preferred_element_type=jnp.float32)
    up = jnp.dot(normed, w_up.T, preferred_element_type=jnp.float32)
    hidden = (jax.nn.silu(gate) * up).astype(jnp.bfloat16)
    down = jnp.dot(hidden, w_down, preferred_element_type=jnp.float32)
    mixed = (carried + down).astype(jnp.bfloat16)
    return mixed.reshape(N_SEQ, GROUPS, SUB, D).transpose(1, 3, 0, 2).reshape(GROUPS, D, N_SEQ * SUB)
```

```python
import functools

import jax
import jax.numpy as jnp
from jax import lax
from jax.experimental import pallas as pl
from jax.experimental.pallas import tpu as pltpu
from jax.sharding import PartitionSpec as P

D = 5120
HEAD_DIM = 128


def key_positions(order, start, count, block_rows):
    row_ids = start + jnp.arange(count, dtype=jnp.int32)
    owners = row_ids // block_rows
    match = owners[:, None] == jnp.arange(order.shape[0], dtype=jnp.int32)[None, :]
    first = jnp.sum(jnp.where(match, order[None, :], 0), axis=1)
    return first * block_rows + row_ids % block_rows


VMEM_BUDGET = 60 * 2**20


class Copies:
    def __init__(self, send_sems):
        self.sems = send_sems
        self.started = []

    def send(self, src, dst, recv_sem, device):
        copy = pltpu.make_async_remote_copy(
            src_ref=src,
            dst_ref=dst,
            send_sem=self.sems.at[len(self.started)],
            recv_sem=recv_sem,
            device_id=device,
            device_id_type=pl.DeviceIdType.MESH,
        )
        copy.start()
        self.started.append(copy)

    def arrived(self, dst, recv_sem, device):
        pltpu.make_async_remote_copy(
            src_ref=dst,
            dst_ref=dst,
            send_sem=self.sems.at[0],
            recv_sem=recv_sem,
            device_id=device,
            device_id_type=pl.DeviceIdType.MESH,
        ).wait_recv()

    def finish(self):
        for copy in self.started:
            copy.wait_send()


def greet(peers):
    barrier = pltpu.get_barrier_semaphore()
    for peer in peers:
        pl.semaphore_signal(barrier, inc=1, device_id=peer, device_id_type=pl.DeviceIdType.MESH)
    pl.semaphore_wait(barrier, len(peers))


def mlp_kernel(
    n_seq, scaled_ref, squares_ref, carried_ref, w_gate_hbm, w_up_hbm, w_down_hbm, out_ref,
    x, sq, w_gate, w_up, w_down, gate_acc, up_acc, hidden, part, from_rep, to_y, from_y, to_z, from_z,
    weight_sem, own_sem, send_sem, x_sem, sq_sem, rep_sem, y_sem, z_sem,
):
    section, s, r = lax.axis_index("section"), lax.axis_index("seq"), lax.axis_index("rep")
    depth = n_seq // 2
    tokens, columns = scaled_ref.shape
    half = w_gate.shape[0]
    z, y = s // 2, lax.rem(s, 2)
    other_y, other_r = 1 - y, 1 - r

    def at(z_step, y_index):
        return lax.rem(z + z_step, depth) * 2 + y_index

    def dev(seq_index, rep_index):
        return (section, seq_index, rep_index)

    rep_mate, y_mate = dev(s, other_r), dev(at(0, other_y), r)
    loads = []
    for i, (hbm, vmem) in enumerate(((w_gate_hbm, w_gate), (w_up_hbm, w_up), (w_down_hbm, w_down))):
        load = pltpu.make_async_copy(hbm.at[pl.ds(r * half, half), :], vmem, weight_sem.at[i])
        load.start()
        loads.append(load)

    def rows(rep_index):
        return pl.ds(rep_index * tokens, tokens)

    own = [
        pltpu.make_async_copy(scaled_ref, x.at[s, rows(r), :], own_sem.at[0]),
        pltpu.make_async_copy(squares_ref, sq.at[s, r], own_sem.at[1]),
    ]
    for copy in own:
        copy.start()
    peers = [
        dev(lax.rem(s + k, n_seq), rep_index)
        for k in range(n_seq)
        for rep_index in (r, other_r)
        if (k, rep_index is r) != (0, True)
    ]
    greet(peers)
    copies = Copies(send_sem)
    for peer in peers:
        copies.send(squares_ref, sq.at[s, r], sq_sem.at[s, r], peer)

    def forward(src, seq_index, device):
        copies.send(src, x.at[seq_index, rows(r), :], x_sem.at[seq_index, r], device)

    forward(scaled_ref, s, y_mate)
    for k in range(1, depth):
        forward(scaled_ref, s, dev(at(k, y), r))
    forward(scaled_ref, s, rep_mate)
    for copy in own:
        copy.wait()

    first = True

    def accumulate(seq_index):
        nonlocal first
        copies.arrived(x.at[seq_index, rows(other_r), :], x_sem.at[seq_index, other_r], rep_mate)
        block = x[seq_index]
        span = pl.ds(pl.multiple_of(seq_index * columns, 128), columns)
        for w, acc, load in ((w_gate, gate_acc, loads[0]), (w_up, up_acc, loads[1])):
            if first:
                load.wait()
            term = lax.dot_general(
                block, w[:, span], (((1,), (1,)), ((), ())), preferred_element_type=jnp.float32
            )
            if first:
                acc[...] = term
            else:
                acc[...] += term
        first = False

    events = []
    for k in range(depth):
        if k:
            events.append((k, 0))
        if k >= 1:
            events.append((k - 1, 1))
    events.append((depth - 1, 1))
    pending = s
    for k, from_mate in events:
        seq_index = at(depth - k, other_y if from_mate else y)
        piece = x.at[seq_index, rows(r), :]
        copies.arrived(piece, x_sem.at[seq_index, r], y_mate)
        if not from_mate:
            forward(piece, seq_index, y_mate)
        forward(piece, seq_index, rep_mate)
        accumulate(pending)
        pending = seq_index
    for k in range(n_seq):
        for rep_index in (r, other_r):
            if (k, rep_index is r) != (0, True):
                seq_index = lax.rem(s + k, n_seq)
                copies.arrived(sq.at[seq_index, rep_index], sq_sem.at[seq_index, rep_index], rep_mate)
    accumulate(pending)

    for rep_index in range(2):
        total = jnp.sum(sq[:, rep_index], axis=0)
        factor = lax.rsqrt(total / (n_seq * columns) + 1e-05)
        factor = jnp.transpose(factor)[:, :1]
        own_rows = slice(rep_index * tokens, (rep_index + 1) * tokens)
        gate = gate_acc[own_rows, :] * factor
        up = up_acc[own_rows, :] * factor
        hidden[own_rows, :] = (gate / (1.0 + jnp.exp(-gate)) * up).astype(jnp.bfloat16)
    loads[2].wait()

    order = [(k % depth, 1) for k in range(1, depth + 1)] + [(k % depth, 0) for k in range(1, depth + 1)]
    slot_of = {step: i for i, step in enumerate(order)}

    def joined(slot):
        return part[slot, rows(r), :] + from_rep[slot]

    def after_rep(slot):
        k, to_mate = order[slot]
        copies.arrived(from_rep.at[slot], rep_sem.at[slot], rep_mate)
        if to_mate:
            to_y[k] = joined(slot).astype(jnp.bfloat16)
            copies.send(to_y.at[k], from_y.at[k], y_sem.at[k], y_mate)

    for slot, (k, to_mate) in enumerate(order):
        seq_index = at(k, other_y if to_mate else y)
        span = pl.ds(pl.multiple_of(seq_index * columns, 128), columns)
        part[slot] = jnp.dot(hidden[...], w_down[:, span], preferred_element_type=jnp.float32)
        copies.send(part.at[slot, rows(other_r), :], from_rep.at[slot], rep_sem.at[slot], rep_mate)
        if slot:
            after_rep(slot - 1)
    after_rep(len(order) - 1)
    for k in range(1, depth):
        copies.arrived(from_y.at[k], y_sem.at[k], y_mate)
        to_z[k - 1] = (joined(slot_of[k, 0]) + from_y[k].astype(jnp.float32)).astype(jnp.bfloat16)
        copies.send(to_z.at[k - 1], from_z.at[k - 1], z_sem.at[k - 1], dev(at(k, y), r))
    copies.arrived(from_y.at[0], y_sem.at[0], y_mate)
    total = carried_ref[...] + joined(slot_of[0, 0]) + from_y[0].astype(jnp.float32)
    for k in range(1, depth):
        copies.arrived(from_z.at[k - 1], z_sem.at[k - 1], y_mate)
        total += from_z[k - 1].astype(jnp.float32)
    out_ref[...] = total.astype(jnp.bfloat16)
    copies.finish()


def mlp(scaled, squares, carried, w_gate, w_up, w_down):
    n_seq, n_rep = lax.axis_size("seq"), lax.axis_size("rep")
    tokens, columns = scaled.shape
    features = w_gate.shape[1]
    half = w_gate.shape[0] // n_rep
    depth = n_seq // 2
    sends = n_seq * n_rep + (depth + 1) + 2 * n_seq + 2 * n_seq + 2 * depth
    f32, bf16 = jnp.float32, jnp.bfloat16
    vmem = pl.BlockSpec(memory_space=pltpu.VMEM)
    hbm = pl.BlockSpec(memory_space=pl.ANY)
    dma = pltpu.SemaphoreType.DMA
    return pl.pallas_call(
        functools.partial(mlp_kernel, n_seq),
        out_shape=jax.ShapeDtypeStruct((tokens, columns), bf16),
        in_specs=[vmem, vmem, vmem, hbm, hbm, hbm],
        out_specs=vmem,
        scratch_shapes=[
            pltpu.VMEM((n_seq, n_rep * tokens, columns), bf16),
            pltpu.VMEM((n_seq, n_rep, 8, tokens), f32),
            pltpu.VMEM((half, features), bf16),
            pltpu.VMEM((half, features), bf16),
            pltpu.VMEM((half, features), bf16),
            pltpu.VMEM((n_rep * tokens, half), f32),
            pltpu.VMEM((n_rep * tokens, half), f32),
            pltpu.VMEM((n_rep * tokens, half), bf16),
            pltpu.VMEM((n_seq, n_rep * tokens, columns), f32),
            pltpu.VMEM((n_seq, tokens, columns), f32),
            pltpu.VMEM((depth, tokens, columns), bf16),
            pltpu.VMEM((depth, tokens, columns), bf16),
            pltpu.VMEM((depth - 1, tokens, columns), bf16),
            pltpu.VMEM((depth - 1, tokens, columns), bf16),
            dma((3,)),
            dma((2,)),
            dma((sends,)),
            dma((n_seq, n_rep)),
            dma((n_seq, n_rep)),
            dma((n_seq,)),
            dma((depth,)),
            dma((depth - 1,)),
        ],
        compiler_params=pltpu.CompilerParams(
            collective_id=1, has_side_effects=True, vmem_limit_bytes=VMEM_BUDGET
        ),
    )(scaled, squares, carried, w_gate, w_up, w_down)


def kernels_fit(wo, w_gate, tokens):
    n_seq, n_rep = lax.axis_size("seq"), lax.axis_size("rep")
    columns = wo.shape[1]
    half = w_gate.shape[0] // n_rep
    held = 3 * half * w_gate.shape[1] * 2 + n_seq * tokens * columns * 16 + 20 * tokens * half
    return (
        n_rep == 2
        and n_seq % 2 == 0
        and n_seq >= 4
        and columns % 128 == 0
        and tokens % 128 == 0
        and w_gate.shape[0] % (16 * n_rep) == 0
        and held < VMEM_BUDGET - 8 * 2**20
    )


def on_device(queries, keys, values, block_order, wo, resid, gain, w_gate, w_up, w_down):
    seq_dev = queries.shape[0]
    heads_dev = queries.shape[1] // HEAD_DIM
    groups = lax.axis_size("section") * lax.axis_size("rep")
    n_seq = lax.axis_size("seq")
    sub_rows = seq_dev // groups
    block_rows = seq_dev // 2
    query_start = lax.axis_index("seq") * seq_dev
    query_pos = key_positions(block_order, query_start, seq_dev, block_rows)
    query_heads = queries.reshape(seq_dev, heads_dev, HEAD_DIM)
    scale = HEAD_DIM ** (-0.5)
    running_max = jnp.full((seq_dev, heads_dev), -1e30, jnp.float32)
    key_piece = lax.all_gather(keys, "seq", axis=0, tiled=True)
    value_piece = lax.all_gather(values, "seq", axis=0, tiled=True)
    count = key_piece.shape[0]
    key_pos = key_positions(block_order, jnp.int32(0), count, block_rows)
    scores = (
        jnp.einsum(
            "qhd,khd->qhk",
            query_heads,
            key_piece.reshape(count, heads_dev, HEAD_DIM),
            preferred_element_type=jnp.float32,
        )
        * scale
    )
    visible = (key_pos[None, :] <= query_pos[:, None])[:, None, :]
    new_max = jnp.maximum(running_max, jnp.max(jnp.where(visible, scores, -1e30), axis=-1))
    probs = jnp.where(visible, jnp.exp(scores - new_max[..., None]), 0.0)
    total = jnp.sum(probs, axis=-1)
    weighted = jnp.einsum(
        "qhk,khd->qhd",
        probs.astype(jnp.bfloat16),
        value_piece.reshape(count, heads_dev, HEAD_DIM),
        preferred_element_type=jnp.float32,
    )
    running_max, total, weighted = (new_max, total, weighted)
    attended = (
        (weighted / total[..., None]).astype(jnp.bfloat16).reshape(seq_dev, heads_dev * HEAD_DIM)
    )
    columns = wo.shape[1]
    token_count = n_seq * sub_rows
    parts = attended.reshape(groups, sub_rows, heads_dev * HEAD_DIM)
    group_rows = lax.all_to_all(parts, ("section", "rep"), split_axis=0, concat_axis=2, tiled=True)
    wo_columns = lax.all_gather(wo, ("section", "rep"), axis=0, tiled=True)
    piece = lax.all_gather(group_rows, "seq", axis=0, tiled=True)
    flat = piece.reshape(piece.shape[0] * piece.shape[1], piece.shape[2])
    product = jnp.dot(flat, wo_columns, preferred_element_type=jnp.float32)
    projected = product.reshape(piece.shape[0], piece.shape[1], columns)
    if kernels_fit(wo, w_gate, token_count):
        base = resid.reshape(columns, token_count).T.astype(jnp.float32)
        carried = base + projected.reshape(token_count, columns)
        squares = jnp.broadcast_to(jnp.sum(carried * carried, axis=1)[None, :], (8, token_count))
        scaled = (carried * gain.astype(jnp.float32)[None, :]).astype(jnp.bfloat16)
        mixed = mlp(scaled, squares, carried, w_gate, w_up, w_down)
        return mixed.T.reshape(resid.shape)
    projected_cols = projected.reshape(token_count, columns).T
    carried = resid.reshape(columns, token_count).astype(jnp.float32) + projected_cols
    squares = lax.psum(jnp.sum(carried * carried, axis=0), "seq")
    normed = (
        carried * lax.rsqrt(squares / D + 1e-05)[None, :] * gain.astype(jnp.float32)[:, None]
    ).astype(jnp.bfloat16)
    piece = lax.all_gather(normed, "seq", axis=0, tiled=True)
    gate_sum = jnp.dot(w_gate, piece, preferred_element_type=jnp.float32)
    up_sum = jnp.dot(w_up, piece, preferred_element_type=jnp.float32)
    hidden = (jax.nn.silu(gate_sum) * up_sum).astype(jnp.bfloat16)
    term = lax.dot_general(
        w_down, hidden, (((0,), (0,)), ((), ())), preferred_element_type=jnp.float32
    )
    down = lax.psum_scatter(term, "seq", scatter_dimension=0, tiled=True)
    return (carried + down).astype(jnp.bfloat16).reshape(resid.shape)


def solution(mesh):
    return jax.shard_map(
        on_device,
        mesh=mesh,
        in_specs=(
            P("seq", ("section", "rep")),
            P("seq", ("section", "rep")),
            P("seq", ("section", "rep")),
            P(),
            P(("section", "rep"), "seq"),
            P(("section", "rep"), "seq", None),
            P("seq"),
            P("seq", None),
            P("seq", None),
            P("seq", None),
        ),
        out_specs=P(("section", "rep"), "seq", None),
        check_vma=False,
    )
```

```python
import functools

import jax
import jax.numpy as jnp
from jax import lax
from jax.experimental import pallas as pl
from jax.experimental.pallas import tpu as pltpu
from jax.sharding import PartitionSpec as P

D = 5120
HEAD_DIM = 128


def key_positions(order, start, count, block_rows):
    row_ids = start + jnp.arange(count, dtype=jnp.int32)
    owners = row_ids // block_rows
    match = owners[:, None] == jnp.arange(order.shape[0], dtype=jnp.int32)[None, :]
    first = jnp.sum(jnp.where(match, order[None, :], 0), axis=1)
    return first * block_rows + row_ids % block_rows


VMEM_BUDGET = 60 * 2**20


class Copies:
    def __init__(self, send_sems):
        self.sems = send_sems
        self.started = []

    def send(self, src, dst, recv_sem, device):
        copy = pltpu.make_async_remote_copy(
            src_ref=src,
            dst_ref=dst,
            send_sem=self.sems.at[len(self.started)],
            recv_sem=recv_sem,
            device_id=device,
            device_id_type=pl.DeviceIdType.MESH,
        )
        copy.start()
        self.started.append(copy)

    def arrived(self, dst, recv_sem, device):
        pltpu.make_async_remote_copy(
            src_ref=dst,
            dst_ref=dst,
            send_sem=self.sems.at[0],
            recv_sem=recv_sem,
            device_id=device,
            device_id_type=pl.DeviceIdType.MESH,
        ).wait_recv()

    def finish(self):
        for copy in self.started:
            copy.wait_send()


def greet(peers):
    barrier = pltpu.get_barrier_semaphore()
    for peer in peers:
        pl.semaphore_signal(barrier, inc=1, device_id=peer, device_id_type=pl.DeviceIdType.MESH)
    pl.semaphore_wait(barrier, len(peers))


def layer_kernel(
    n_seq, n_rep, groups,
    q_ref, k_ref, v_ref, bias_ref, wo_ref, base_ref, gain_ref, w_gate_hbm, w_up_hbm, w_down_hbm, out_ref,
    keys, values, attended, proj, proj_low, from_group, carried,
    x, sq, w_gate, w_up, w_down, gate_acc, up_acc, hidden, part, from_rep, to_y, from_y, to_z, from_z,
    weight_sem, own_sem, send_sem, k_sem, v_sem, att_sem, group_sem, x_sem, sq_sem, rep_sem, y_sem, z_sem,
):
    section, s, r = lax.axis_index("section"), lax.axis_index("seq"), lax.axis_index("rep")
    depth = n_seq // 2
    tokens, columns = base_ref.shape
    seq_dev = q_ref.shape[0]
    sub = seq_dev // groups
    half = w_gate.shape[0]
    z, y = s // 2, lax.rem(s, 2)
    other_y, other_r = 1 - y, 1 - r
    group = section * n_rep + r

    def at(z_step, y_index):
        return lax.rem(z + z_step, depth) * 2 + y_index

    def dev(seq_index, rep_index):
        return (section, seq_index, rep_index)

    def group_dev(step):
        other = lax.rem(group + step, groups)
        return (other // n_rep, s, lax.rem(other, n_rep))

    rep_mate, y_mate = dev(s, other_r), dev(at(0, other_y), r)
    loads = []
    for i, (hbm, vmem) in enumerate(((w_gate_hbm, w_gate), (w_up_hbm, w_up), (w_down_hbm, w_down))):
        load = pltpu.make_async_copy(hbm.at[pl.ds(r * half, half), :], vmem, weight_sem.at[i])
        load.start()
        loads.append(load)

    def rows(rep_index):
        return pl.ds(rep_index * tokens, tokens)

    own = [
        pltpu.make_async_copy(k_ref, keys.at[s], own_sem.at[0]),
        pltpu.make_async_copy(v_ref, values.at[s], own_sem.at[1]),
    ]
    for copy in own:
        copy.start()
    peers = [
        dev(lax.rem(s + k, n_seq), rep_index)
        for k in range(n_seq)
        for rep_index in (r, other_r)
        if (k, rep_index is r) != (0, True)
    ]
    greet(peers + [(lax.rem(section + k, groups // n_rep), s, i) for k in range(1, groups // n_rep) for i in range(n_rep)])
    copies = Copies(send_sem)

    def spread(src, dst, sem):
        copies.send(src, dst.at[s], sem.at[s], y_mate)
        for k in range(1, depth):
            copies.send(src, dst.at[s], sem.at[s], dev(at(k, y), r))

    def take(dst, sem, k, from_mate):
        seq_index = at(depth - k, other_y if from_mate else y)
        copies.arrived(dst.at[seq_index], sem.at[seq_index], y_mate)
        if not from_mate:
            copies.send(dst.at[seq_index], dst.at[seq_index], sem.at[seq_index], y_mate)
        return seq_index

    events = []
    for k in range(depth):
        if k:
            events.append((k, 0))
            events.append((k - 1, 1))
    events.append((depth - 1, 1))

    spread(k_ref, keys, k_sem)
    spread(v_ref, values, v_sem)
    for k in range(1, depth):
        take(keys, k_sem, k, 0)
    for k in range(1, depth):
        take(values, v_sem, k, 0)
    for copy in own:
        copy.wait()
    for k in range(depth):
        take(keys, k_sem, k, 1)
    heads = q_ref.shape[1] // HEAD_DIM
    all_keys = keys.reshape(n_seq * seq_dev, q_ref.shape[1])
    all_values = values.reshape(n_seq * seq_dev, q_ref.shape[1])
    probs, totals = [], []
    for h in range(heads):
        span = slice(h * HEAD_DIM, (h + 1) * HEAD_DIM)
        scores = lax.dot_general(
            q_ref[:, span], all_keys[:, span], (((1,), (1,)), ((), ())), preferred_element_type=jnp.float32
        )
        scores = scores * HEAD_DIM**-0.5 + bias_ref[...]
        prob = jnp.exp(scores - jnp.max(scores, axis=1, keepdims=True))
        totals.append(jnp.sum(prob, axis=1, keepdims=True))
        probs.append(prob.astype(jnp.bfloat16))
    for k in range(depth):
        take(values, v_sem, k, 1)
    for h in range(heads):
        span = slice(h * HEAD_DIM, (h + 1) * HEAD_DIM)
        weighted = jnp.dot(probs[h], all_values[:, span], preferred_element_type=jnp.float32)
        attended[s, :, span] = (weighted / totals[h]).astype(jnp.bfloat16)
    spread(attended.at[s], attended, att_sem)

    def project(seq_index):
        proj[...] = jnp.dot(attended[seq_index], wo_ref[...], preferred_element_type=jnp.float32)
        proj_low[seq_index] = proj[...].astype(jnp.bfloat16)
        spot = pl.ds(pl.multiple_of(seq_index * sub, sub), sub)
        carried[spot, :] = base_ref[spot, :] + proj[pl.ds(pl.multiple_of(group * sub, sub), sub), :]
        for step in range(1, groups):
            other = lax.rem(group + step, groups)
            copies.send(
                proj_low.at[seq_index, pl.ds(pl.multiple_of(other * sub, sub), sub), :],
                from_group.at[step - 1, spot, :],
                group_sem.at[step - 1, seq_index],
                group_dev(step),
            )

    pending = s
    for k, from_mate in events:
        seq_index = take(attended, att_sem, k, from_mate)
        project(pending)
        pending = seq_index
    project(pending)
    for step in range(1, groups):
        for k in range(n_seq):
            spot = pl.ds(k * sub, sub)
            copies.arrived(from_group.at[step - 1, spot, :], group_sem.at[step - 1, k], rep_mate)
    total = carried[...]
    for step in range(1, groups):
        total += from_group[step - 1].astype(jnp.float32)
    carried[...] = total
    squares = jnp.sum(total * total, axis=1, keepdims=True)
    sq[s, r] = jnp.transpose(jnp.broadcast_to(squares, (tokens, tokens)))[:8]
    x[s, rows(r), :] = (total * gain_ref[...]).astype(jnp.bfloat16)
    for peer in peers:
        copies.send(sq.at[s, r], sq.at[s, r], sq_sem.at[s, r], peer)

    def forward(seq_index, device):
        piece = x.at[seq_index, rows(r), :]
        copies.send(piece, piece, x_sem.at[seq_index, r], device)

    forward(s, y_mate)
    for k in range(1, depth):
        forward(s, dev(at(k, y), r))
    forward(s, rep_mate)

    first = True

    def accumulate(seq_index):
        nonlocal first
        copies.arrived(x.at[seq_index, rows(other_r), :], x_sem.at[seq_index, other_r], rep_mate)
        block = x[seq_index]
        span = pl.ds(pl.multiple_of(seq_index * columns, 128), columns)
        for w, acc, load in ((w_gate, gate_acc, loads[0]), (w_up, up_acc, loads[1])):
            if first:
                load.wait()
            term = lax.dot_general(
                block, w[:, span], (((1,), (1,)), ((), ())), preferred_element_type=jnp.float32
            )
            if first:
                acc[...] = term
            else:
                acc[...] += term
        first = False

    pending = s
    for k, from_mate in events:
        seq_index = at(depth - k, other_y if from_mate else y)
        piece = x.at[seq_index, rows(r), :]
        copies.arrived(piece, x_sem.at[seq_index, r], y_mate)
        if not from_mate:
            forward(seq_index, y_mate)
        forward(seq_index, rep_mate)
        accumulate(pending)
        pending = seq_index
    for k in range(n_seq):
        for rep_index in (r, other_r):
            if (k, rep_index is r) != (0, True):
                seq_index = lax.rem(s + k, n_seq)
                copies.arrived(sq.at[seq_index, rep_index], sq_sem.at[seq_index, rep_index], rep_mate)
    accumulate(pending)

    for rep_index in range(2):
        total = jnp.sum(sq[:, rep_index], axis=0)
        factor = lax.rsqrt(total / (n_seq * columns) + 1e-05)
        factor = jnp.transpose(factor)[:, :1]
        own_rows = slice(rep_index * tokens, (rep_index + 1) * tokens)
        gate = gate_acc[own_rows, :] * factor
        up = up_acc[own_rows, :] * factor
        hidden[own_rows, :] = (gate / (1.0 + jnp.exp(-gate)) * up).astype(jnp.bfloat16)
    loads[2].wait()

    order = [(k % depth, 1) for k in range(1, depth + 1)] + [(k % depth, 0) for k in range(1, depth + 1)]
    slot_of = {step: i for i, step in enumerate(order)}

    def joined(slot):
        return part[slot, rows(r), :] + from_rep[slot]

    def after_rep(slot):
        k, to_mate = order[slot]
        copies.arrived(from_rep.at[slot], rep_sem.at[slot], rep_mate)
        if to_mate:
            to_y[k] = joined(slot).astype(jnp.bfloat16)
            copies.send(to_y.at[k], from_y.at[k], y_sem.at[k], y_mate)

    for slot, (k, to_mate) in enumerate(order):
        seq_index = at(k, other_y if to_mate else y)
        span = pl.ds(pl.multiple_of(seq_index * columns, 128), columns)
        part[slot] = jnp.dot(hidden[...], w_down[:, span], preferred_element_type=jnp.float32)
        copies.send(part.at[slot, rows(other_r), :], from_rep.at[slot], rep_sem.at[slot], rep_mate)
        if slot:
            after_rep(slot - 1)
    after_rep(len(order) - 1)
    for k in range(1, depth):
        copies.arrived(from_y.at[k], y_sem.at[k], y_mate)
        to_z[k - 1] = (joined(slot_of[k, 0]) + from_y[k].astype(jnp.float32)).astype(jnp.bfloat16)
        copies.send(to_z.at[k - 1], from_z.at[k - 1], z_sem.at[k - 1], dev(at(k, y), r))
    copies.arrived(from_y.at[0], y_sem.at[0], y_mate)
    total = carried[...] + joined(slot_of[0, 0]) + from_y[0].astype(jnp.float32)
    for k in range(1, depth):
        copies.arrived(from_z.at[k - 1], z_sem.at[k - 1], y_mate)
        total += from_z[k - 1].astype(jnp.float32)
    out_ref[...] = total.astype(jnp.bfloat16)
    copies.finish()


def layer(q, k, v, bias, wo, base, gain, w_gate, w_up, w_down):
    n_seq, n_rep = lax.axis_size("seq"), lax.axis_size("rep")
    groups = n_rep * lax.axis_size("section")
    seq_dev, width = q.shape
    tokens, columns = base.shape
    features = w_gate.shape[1]
    half = w_gate.shape[0] // n_rep
    depth = n_seq // 2
    sends = 3 * (n_seq - 1) + n_seq * (groups - 1) + (2 * n_seq - 1) * 2 + 2 * n_seq
    f32, bf16 = jnp.float32, jnp.bfloat16
    vmem = pl.BlockSpec(memory_space=pltpu.VMEM)
    hbm = pl.BlockSpec(memory_space=pl.ANY)
    dma = pltpu.SemaphoreType.DMA
    return pl.pallas_call(
        functools.partial(layer_kernel, n_seq, n_rep, groups),
        out_shape=jax.ShapeDtypeStruct((tokens, columns), bf16),
        in_specs=[vmem] * 7 + [hbm] * 3,
        out_specs=vmem,
        scratch_shapes=[
            pltpu.VMEM((n_seq, seq_dev, width), bf16),
            pltpu.VMEM((n_seq, seq_dev, width), bf16),
            pltpu.VMEM((n_seq, seq_dev, width), bf16),
            pltpu.VMEM((seq_dev, columns), f32),
            pltpu.VMEM((n_seq, seq_dev, columns), bf16),
            pltpu.VMEM((groups - 1, tokens, columns), bf16),
            pltpu.VMEM((tokens, columns), f32),
            pltpu.VMEM((n_seq, n_rep * tokens, columns), bf16),
            pltpu.VMEM((n_seq, n_rep, 8, tokens), f32),
            pltpu.VMEM((half, features), bf16),
            pltpu.VMEM((half, features), bf16),
            pltpu.VMEM((half, features), bf16),
            pltpu.VMEM((n_rep * tokens, half), f32),
            pltpu.VMEM((n_rep * tokens, half), f32),
            pltpu.VMEM((n_rep * tokens, half), bf16),
            pltpu.VMEM((n_seq, n_rep * tokens, columns), f32),
            pltpu.VMEM((n_seq, tokens, columns), f32),
            pltpu.VMEM((depth, tokens, columns), bf16),
            pltpu.VMEM((depth, tokens, columns), bf16),
            pltpu.VMEM((depth - 1, tokens, columns), bf16),
            pltpu.VMEM((depth - 1, tokens, columns), bf16),
            dma((3,)),
            dma((2,)),
            dma((sends,)),
            dma((n_seq,)),
            dma((n_seq,)),
            dma((n_seq,)),
            dma((groups - 1, n_seq)),
            dma((n_seq, n_rep)),
            dma((n_seq, n_rep)),
            dma((n_seq,)),
            dma((depth,)),
            dma((depth - 1,)),
        ],
        compiler_params=pltpu.CompilerParams(
            collective_id=1, has_side_effects=True, vmem_limit_bytes=VMEM_BUDGET
        ),
    )(q, k, v, bias, wo, base, gain, w_gate, w_up, w_down)


def kernels_fit(queries, wo, w_gate):
    n_seq, n_rep = lax.axis_size("seq"), lax.axis_size("rep")
    columns = wo.shape[1]
    sub = queries.shape[0] // (n_rep * lax.axis_size("section"))
    tokens = n_seq * sub
    half = w_gate.shape[0] // n_rep
    held = 3 * half * w_gate.shape[1] * 2 + n_seq * tokens * columns * 18 + 20 * tokens * half
    return (
        n_rep == 2
        and n_seq % 2 == 0
        and n_seq >= 4
        and columns % 128 == 0
        and tokens % 128 == 0
        and sub % 16 == 0
        and half % 16 == 0
        and held < VMEM_BUDGET - 8 * 2**20
    )


def on_device(queries, keys, values, block_order, wo, resid, gain, w_gate, w_up, w_down):
    seq_dev = queries.shape[0]
    heads_dev = queries.shape[1] // HEAD_DIM
    groups = lax.axis_size("section") * lax.axis_size("rep")
    n_seq = lax.axis_size("seq")
    sub_rows = seq_dev // groups
    block_rows = seq_dev // 2
    query_start = lax.axis_index("seq") * seq_dev
    query_pos = key_positions(block_order, query_start, seq_dev, block_rows)
    if kernels_fit(queries, wo, w_gate):
        key_pos = key_positions(block_order, jnp.int32(0), n_seq * seq_dev, block_rows)
        bias = jnp.where(key_pos[None, :] <= query_pos[:, None], 0.0, -1e30).astype(jnp.float32)
        base = resid.reshape(wo.shape[1], n_seq * sub_rows).T.astype(jnp.float32)
        gain_row = gain.astype(jnp.float32)[None, :]
        mixed = layer(queries, keys, values, bias, wo, base, gain_row, w_gate, w_up, w_down)
        return mixed.T.reshape(resid.shape)
    query_heads = queries.reshape(seq_dev, heads_dev, HEAD_DIM)
    scale = HEAD_DIM ** (-0.5)
    running_max = jnp.full((seq_dev, heads_dev), -1e30, jnp.float32)
    key_piece = lax.all_gather(keys, "seq", axis=0, tiled=True)
    value_piece = lax.all_gather(values, "seq", axis=0, tiled=True)
    count = key_piece.shape[0]
    key_pos = key_positions(block_order, jnp.int32(0), count, block_rows)
    scores = (
        jnp.einsum(
            "qhd,khd->qhk",
            query_heads,
            key_piece.reshape(count, heads_dev, HEAD_DIM),
            preferred_element_type=jnp.float32,
        )
        * scale
    )
    visible = (key_pos[None, :] <= query_pos[:, None])[:, None, :]
    new_max = jnp.maximum(running_max, jnp.max(jnp.where(visible, scores, -1e30), axis=-1))
    probs = jnp.where(visible, jnp.exp(scores - new_max[..., None]), 0.0)
    total = jnp.sum(probs, axis=-1)
    weighted = jnp.einsum(
        "qhk,khd->qhd",
        probs.astype(jnp.bfloat16),
        value_piece.reshape(count, heads_dev, HEAD_DIM),
        preferred_element_type=jnp.float32,
    )
    running_max, total, weighted = (new_max, total, weighted)
    attended = (
        (weighted / total[..., None]).astype(jnp.bfloat16).reshape(seq_dev, heads_dev * HEAD_DIM)
    )
    columns = wo.shape[1]
    token_count = n_seq * sub_rows
    parts = attended.reshape(groups, sub_rows, heads_dev * HEAD_DIM)
    group_rows = lax.all_to_all(parts, ("section", "rep"), split_axis=0, concat_axis=2, tiled=True)
    wo_columns = lax.all_gather(wo, ("section", "rep"), axis=0, tiled=True)
    piece = lax.all_gather(group_rows, "seq", axis=0, tiled=True)
    flat = piece.reshape(piece.shape[0] * piece.shape[1], piece.shape[2])
    product = jnp.dot(flat, wo_columns, preferred_element_type=jnp.float32)
    projected = product.reshape(piece.shape[0], piece.shape[1], columns)
    projected_cols = projected.reshape(token_count, columns).T
    carried = resid.reshape(columns, token_count).astype(jnp.float32) + projected_cols
    squares = lax.psum(jnp.sum(carried * carried, axis=0), "seq")
    normed = (
        carried * lax.rsqrt(squares / D + 1e-05)[None, :] * gain.astype(jnp.float32)[:, None]
    ).astype(jnp.bfloat16)
    piece = lax.all_gather(normed, "seq", axis=0, tiled=True)
    gate_sum = jnp.dot(w_gate, piece, preferred_element_type=jnp.float32)
    up_sum = jnp.dot(w_up, piece, preferred_element_type=jnp.float32)
    hidden = (jax.nn.silu(gate_sum) * up_sum).astype(jnp.bfloat16)
    term = lax.dot_general(
        w_down, hidden, (((0,), (0,)), ((), ())), preferred_element_type=jnp.float32
    )
    down = lax.psum_scatter(term, "seq", scatter_dimension=0, tiled=True)
    return (carried + down).astype(jnp.bfloat16).reshape(resid.shape)


def solution(mesh):
    return jax.shard_map(
        on_device,
        mesh=mesh,
        in_specs=(
            P("seq", ("section", "rep")),
            P("seq", ("section", "rep")),
            P("seq", ("section", "rep")),
            P(),
            P(("section", "rep"), "seq"),
            P(("section", "rep"), "seq", None),
            P("seq"),
            P("seq", None),
            P("seq", None),
            P("seq", None),
        ),
        out_specs=P(("section", "rep"), "seq", None),
        check_vma=False,
    )
```

```python
import functools

import jax
import jax.numpy as jnp
from jax import lax
from jax.experimental import pallas as pl
from jax.experimental.pallas import tpu as pltpu
from jax.sharding import PartitionSpec as P

D = 5120
HEAD_DIM = 128


def key_positions(order, start, count, block_rows):
    row_ids = start + jnp.arange(count, dtype=jnp.int32)
    owners = row_ids // block_rows
    match = owners[:, None] == jnp.arange(order.shape[0], dtype=jnp.int32)[None, :]
    first = jnp.sum(jnp.where(match, order[None, :], 0), axis=1)
    return first * block_rows + row_ids % block_rows


VMEM_BUDGET = 60 * 2**20


class Copies:
    def __init__(self, send_sems):
        self.sems = send_sems
        self.started = []

    def send(self, src, dst, recv_sem, device, when=None):
        copy = pltpu.make_async_remote_copy(
            src_ref=src,
            dst_ref=dst,
            send_sem=self.sems.at[len(self.started)],
            recv_sem=recv_sem,
            device_id=device,
            device_id_type=pl.DeviceIdType.MESH,
        )
        if when is None:
            copy.start()
        else:
            pl.when(when)(copy.start)
        self.started.append((copy, when))

    def arrived(self, dst, recv_sem, device):
        pltpu.make_async_remote_copy(
            src_ref=dst,
            dst_ref=dst,
            send_sem=self.sems.at[0],
            recv_sem=recv_sem,
            device_id=device,
            device_id_type=pl.DeviceIdType.MESH,
        ).wait_recv()

    def finish(self):
        for copy, when in self.started:
            if when is None:
                copy.wait_send()
            else:
                pl.when(when)(copy.wait_send)


def greet(peers):
    barrier = pltpu.get_barrier_semaphore()
    for peer in peers:
        pl.semaphore_signal(barrier, inc=1, device_id=peer, device_id_type=pl.DeviceIdType.MESH)
    pl.semaphore_wait(barrier, len(peers))


def mask_bias(order_ref, s, rows, count, block_rows):
    row = lax.broadcasted_iota(jnp.int32, (rows, count), 0)
    column = lax.broadcasted_iota(jnp.int32, (1, count), 1)
    second = row >= block_rows
    row_pos = jnp.where(second, order_ref[2 * s + 1], order_ref[2 * s]) * block_rows
    row_pos += jnp.where(second, row - block_rows, row)
    column_pos = jnp.zeros((1, count), jnp.int32)
    for b in range(count // block_rows):
        column_pos = jnp.where(column >= b * block_rows, (order_ref[b] - b) * block_rows + column, column_pos)
    return jnp.where(column_pos <= row_pos, 0.0, -1e30).astype(jnp.float32)


def layer_kernel(
    n_seq, n_rep, groups,
    order_ref, q_ref, k_ref, v_ref, wo_ref, resid_ref, gain_ref, w_gate_hbm, w_up_hbm, w_down_hbm, out_ref,
    keys, values, attended, bias, proj, proj_low, from_group, carried,
    x, sq, w_gate, w_up, w_down, gate_acc, up_acc, hidden, part, from_rep, to_y, from_y, to_z, from_z,
    weight_sem, own_sem, send_sem, k_sem, v_sem, att_sem, group_sem, x_sem, sq_sem, rep_sem, y_sem, z_sem,
):
    section, s, r = lax.axis_index("section"), lax.axis_index("seq"), lax.axis_index("rep")
    depth = n_seq // 2
    columns, tokens = resid_ref.shape
    seq_dev = q_ref.shape[0]
    block_rows = seq_dev // 2
    sub = seq_dev // groups
    half = w_gate.shape[0]
    z, y = s // 2, lax.rem(s, 2)
    other_y, other_r = 1 - y, 1 - r
    group = section * n_rep + r

    def at(z_step, y_index):
        return lax.rem(z + z_step, depth) * 2 + y_index

    def dev(seq_index, rep_index):
        return (section, seq_index, rep_index)

    def nearest(step):
        near = z + (step + 1) // 2 * (1 if step % 2 == 0 else -1)
        far = jnp.where(2 * z < depth - 1, step, depth - 1 - step)
        return jnp.where(step <= 2 * jnp.minimum(z, depth - 1 - z), near, far)

    sources = [z] + [nearest(step) for step in range(1, depth)]
    above, below = jnp.minimum(z + 1, depth - 1), jnp.maximum(z - 1, 0)

    def group_dev(step):
        other = lax.rem(group + step, groups)
        return (other // n_rep, s, lax.rem(other, n_rep))

    rep_mate, y_mate = dev(s, other_r), dev(at(0, other_y), r)
    loads = []
    for i, (hbm, vmem) in enumerate(((w_gate_hbm, w_gate), (w_up_hbm, w_up), (w_down_hbm, w_down))):
        load = pltpu.make_async_copy(hbm.at[pl.ds(r * half, half), :], vmem, weight_sem.at[i])
        load.start()
        loads.append(load)

    def rows(rep_index):
        return pl.ds(rep_index * tokens, tokens)

    own = [
        pltpu.make_async_copy(k_ref, keys.at[s], own_sem.at[0]),
        pltpu.make_async_copy(v_ref, values.at[s], own_sem.at[1]),
    ]
    for copy in own:
        copy.start()
    peers = [
        dev(lax.rem(s + k, n_seq), rep_index)
        for k in range(n_seq)
        for rep_index in (r, other_r)
        if (k, rep_index is r) != (0, True)
    ]
    greet(peers + [(lax.rem(section + k, groups // n_rep), s, i) for k in range(1, groups // n_rep) for i in range(n_rep)])
    copies = Copies(send_sem)

    def along(src, dst, sem):
        copies.send(src, dst, sem, dev(above * 2 + y, r), when=z < depth - 1)
        copies.send(src, dst, sem, dev(below * 2 + y, r), when=z > 0)

    def onward(piece, sem, source):
        up = source < z
        device = dev(jnp.where(up, above, below) * 2 + y, r)
        more = jnp.where(up, z < depth - 1, z > 0)
        copies.send(piece, piece, sem, device, when=more)

    def spread(src, dst, sem):
        along(src, dst.at[s], sem.at[s])
        copies.send(src, dst.at[s], sem.at[s], y_mate)

    def take(dst, sem, k, from_mate):
        seq_index = sources[k] * 2 + (other_y if from_mate else y)
        piece = dst.at[seq_index]
        copies.arrived(piece, sem.at[seq_index], y_mate)
        if not from_mate:
            onward(piece, sem.at[seq_index], sources[k])
            copies.send(piece, piece, sem.at[seq_index], y_mate)
        return seq_index

    events = []
    for k in range(depth):
        if k:
            events.append((k, 0))
            events.append((k - 1, 1))
    events.append((depth - 1, 1))

    spread(k_ref, keys, k_sem)
    spread(v_ref, values, v_sem)
    for k in range(1, depth):
        take(keys, k_sem, k, 0)
        take(values, v_sem, k, 0)
        if k == 1:
            carried[...] = jnp.transpose(resid_ref[...].astype(jnp.float32))
            bias[...] = mask_bias(order_ref, s, seq_dev, n_seq * seq_dev, block_rows)
    for copy in own:
        copy.wait()
    for k in range(depth):
        take(keys, k_sem, k, 1)
    heads = q_ref.shape[1] // HEAD_DIM
    all_keys = keys.reshape(n_seq * seq_dev, q_ref.shape[1])
    all_values = values.reshape(n_seq * seq_dev, q_ref.shape[1])
    probs, totals = [], []
    for h in range(heads):
        span = slice(h * HEAD_DIM, (h + 1) * HEAD_DIM)
        scores = lax.dot_general(
            q_ref[:, span], all_keys[:, span], (((1,), (1,)), ((), ())), preferred_element_type=jnp.float32
        )
        scores = scores * HEAD_DIM**-0.5 + bias[...]
        prob = jnp.exp(scores - jnp.max(scores, axis=1, keepdims=True))
        totals.append(jnp.sum(prob, axis=1, keepdims=True))
        probs.append(prob.astype(jnp.bfloat16))
    for k in range(depth):
        take(values, v_sem, k, 1)
    for h in range(heads):
        span = slice(h * HEAD_DIM, (h + 1) * HEAD_DIM)
        weighted = jnp.dot(probs[h], all_values[:, span], preferred_element_type=jnp.float32)
        attended[s, :, span] = (weighted / totals[h]).astype(jnp.bfloat16)
    spread(attended.at[s], attended, att_sem)

    def project(seq_index):
        proj[...] = jnp.dot(attended[seq_index], wo_ref[...], preferred_element_type=jnp.float32)
        proj_low[seq_index] = proj[...].astype(jnp.bfloat16)
        spot = pl.ds(pl.multiple_of(seq_index * sub, sub), sub)
        carried[spot, :] += proj[pl.ds(pl.multiple_of(group * sub, sub), sub), :]
        for step in range(1, groups):
            other = lax.rem(group + step, groups)
            copies.send(
                proj_low.at[seq_index, pl.ds(pl.multiple_of(other * sub, sub), sub), :],
                from_group.at[step - 1, spot, :],
                group_sem.at[step - 1, seq_index],
                group_dev(step),
            )

    pending = s
    for k, from_mate in events:
        seq_index = take(attended, att_sem, k, from_mate)
        project(pending)
        pending = seq_index
    project(pending)
    for step in range(1, groups):
        for k in range(n_seq):
            spot = pl.ds(k * sub, sub)
            copies.arrived(from_group.at[step - 1, spot, :], group_sem.at[step - 1, k], rep_mate)
    total = carried[...]
    for step in range(1, groups):
        total += from_group[step - 1].astype(jnp.float32)
    carried[...] = total
    squares = jnp.sum(total * total, axis=1, keepdims=True)
    sq[s, r] = jnp.transpose(jnp.broadcast_to(squares, (tokens, tokens)))[:8]
    x[s, rows(r), :] = (total * gain_ref[...].astype(jnp.float32).reshape(1, columns)).astype(jnp.bfloat16)
    def forward(seq_index, device):
        piece = x.at[seq_index, rows(r), :]
        copies.send(piece, piece, x_sem.at[seq_index, r], device)

    mine = x.at[s, rows(r), :]
    along(mine, mine, x_sem.at[s, r])
    forward(s, y_mate)
    forward(s, rep_mate)
    for peer in peers:
        copies.send(sq.at[s, r], sq.at[s, r], sq_sem.at[s, r], peer)

    first = True

    def accumulate(seq_index):
        nonlocal first
        copies.arrived(x.at[seq_index, rows(other_r), :], x_sem.at[seq_index, other_r], rep_mate)
        block = x[seq_index]
        span = pl.ds(pl.multiple_of(seq_index * columns, 128), columns)
        for w, acc, load in ((w_gate, gate_acc, loads[0]), (w_up, up_acc, loads[1])):
            if first:
                load.wait()
            term = lax.dot_general(
                block, w[:, span], (((1,), (1,)), ((), ())), preferred_element_type=jnp.float32
            )
            if first:
                acc[...] = term
            else:
                acc[...] += term
        first = False

    pending = s
    for k, from_mate in events:
        seq_index = sources[k] * 2 + (other_y if from_mate else y)
        piece = x.at[seq_index, rows(r), :]
        copies.arrived(piece, x_sem.at[seq_index, r], y_mate)
        if not from_mate:
            onward(piece, x_sem.at[seq_index, r], sources[k])
            forward(seq_index, y_mate)
        forward(seq_index, rep_mate)
        accumulate(pending)
        pending = seq_index
    for k in range(n_seq):
        for rep_index in (r, other_r):
            if (k, rep_index is r) != (0, True):
                seq_index = lax.rem(s + k, n_seq)
                copies.arrived(sq.at[seq_index, rep_index], sq_sem.at[seq_index, rep_index], rep_mate)
    accumulate(pending)

    for rep_index in range(2):
        total = jnp.sum(sq[:, rep_index], axis=0)
        factor = lax.rsqrt(total / (n_seq * columns) + 1e-05)
        factor = jnp.transpose(factor)[:, :1]
        own_rows = slice(rep_index * tokens, (rep_index + 1) * tokens)
        gate = gate_acc[own_rows, :] * factor
        up = up_acc[own_rows, :] * factor
        hidden[own_rows, :] = (gate / (1.0 + jnp.exp(-gate)) * up).astype(jnp.bfloat16)
    loads[2].wait()

    order = [(k % depth, 1) for k in range(1, depth + 1)] + [(k % depth, 0) for k in range(1, depth + 1)]
    slot_of = {step: i for i, step in enumerate(order)}

    def joined(slot):
        return part[slot, rows(r), :] + from_rep[slot]

    def after_rep(slot):
        k, to_mate = order[slot]
        copies.arrived(from_rep.at[slot], rep_sem.at[slot], rep_mate)
        if to_mate:
            to_y[k] = joined(slot).astype(jnp.bfloat16)
            copies.send(to_y.at[k], from_y.at[k], y_sem.at[k], y_mate)

    for slot, (k, to_mate) in enumerate(order):
        seq_index = at(k, other_y if to_mate else y)
        span = pl.ds(pl.multiple_of(seq_index * columns, 128), columns)
        part[slot] = jnp.dot(hidden[...], w_down[:, span], preferred_element_type=jnp.float32)
        copies.send(part.at[slot, rows(other_r), :], from_rep.at[slot], rep_sem.at[slot], rep_mate)
        if slot:
            after_rep(slot - 1)
    after_rep(len(order) - 1)
    for k in range(1, depth):
        copies.arrived(from_y.at[k], y_sem.at[k], y_mate)
        to_z[k - 1] = (joined(slot_of[k, 0]) + from_y[k].astype(jnp.float32)).astype(jnp.bfloat16)
        copies.send(to_z.at[k - 1], from_z.at[k - 1], z_sem.at[k - 1], dev(at(k, y), r))
    copies.arrived(from_y.at[0], y_sem.at[0], y_mate)
    total = carried[...] + joined(slot_of[0, 0]) + from_y[0].astype(jnp.float32)
    for k in range(1, depth):
        copies.arrived(from_z.at[k - 1], z_sem.at[k - 1], y_mate)
        total += from_z[k - 1].astype(jnp.float32)
    out_ref[...] = jnp.transpose(total).astype(jnp.bfloat16)
    copies.finish()


def layer(order, q, k, v, wo, resid, gain, w_gate, w_up, w_down):
    n_seq, n_rep = lax.axis_size("seq"), lax.axis_size("rep")
    groups = n_rep * lax.axis_size("section")
    seq_dev, width = q.shape
    columns, tokens = resid.shape
    features = w_gate.shape[1]
    half = w_gate.shape[0] // n_rep
    depth = n_seq // 2
    sends = 3 * (n_seq + 1) + 2 + n_seq * (groups - 1) + (2 * n_seq - 1) * 2 + 2 * n_seq
    f32, bf16 = jnp.float32, jnp.bfloat16
    vmem = pl.BlockSpec(memory_space=pltpu.VMEM)
    hbm = pl.BlockSpec(memory_space=pl.ANY)
    dma = pltpu.SemaphoreType.DMA
    return pl.pallas_call(
        functools.partial(layer_kernel, n_seq, n_rep, groups),
        out_shape=jax.ShapeDtypeStruct((columns, tokens), bf16),
        in_specs=[pl.BlockSpec(memory_space=pltpu.SMEM)] + [vmem] * 6 + [hbm] * 3,
        out_specs=vmem,
        scratch_shapes=[
            pltpu.VMEM((n_seq, seq_dev, width), bf16),
            pltpu.VMEM((n_seq, seq_dev, width), bf16),
            pltpu.VMEM((n_seq, seq_dev, width), bf16),
            pltpu.VMEM((seq_dev, n_seq * seq_dev), f32),
            pltpu.VMEM((seq_dev, columns), f32),
            pltpu.VMEM((n_seq, seq_dev, columns), bf16),
            pltpu.VMEM((groups - 1, tokens, columns), bf16),
            pltpu.VMEM((tokens, columns), f32),
            pltpu.VMEM((n_seq, n_rep * tokens, columns), bf16),
            pltpu.VMEM((n_seq, n_rep, 8, tokens), f32),
            pltpu.VMEM((half, features), bf16),
            pltpu.VMEM((half, features), bf16),
            pltpu.VMEM((half, features), bf16),
            pltpu.VMEM((n_rep * tokens, half), f32),
            pltpu.VMEM((n_rep * tokens, half), f32),
            pltpu.VMEM((n_rep * tokens, half), bf16),
            pltpu.VMEM((n_seq, n_rep * tokens, columns), f32),
            pltpu.VMEM((n_seq, tokens, columns), f32),
            pltpu.VMEM((depth, tokens, columns), bf16),
            pltpu.VMEM((depth, tokens, columns), bf16),
            pltpu.VMEM((depth - 1, tokens, columns), bf16),
            pltpu.VMEM((depth - 1, tokens, columns), bf16),
            dma((3,)),
            dma((2,)),
            dma((sends,)),
            dma((n_seq,)),
            dma((n_seq,)),
            dma((n_seq,)),
            dma((groups - 1, n_seq)),
            dma((n_seq, n_rep)),
            dma((n_seq, n_rep)),
            dma((n_seq,)),
            dma((depth,)),
            dma((depth - 1,)),
        ],
        compiler_params=pltpu.CompilerParams(
            collective_id=1, has_side_effects=True, vmem_limit_bytes=VMEM_BUDGET
        ),
    )(order, q, k, v, wo, resid, gain, w_gate, w_up, w_down)


def kernels_fit(queries, wo, w_gate):
    n_seq, n_rep = lax.axis_size("seq"), lax.axis_size("rep")
    columns = wo.shape[1]
    sub = queries.shape[0] // (n_rep * lax.axis_size("section"))
    tokens = n_seq * sub
    half = w_gate.shape[0] // n_rep
    held = 3 * half * w_gate.shape[1] * 2 + n_seq * tokens * columns * 18 + 20 * tokens * half
    return (
        n_rep == 2
        and n_seq % 2 == 0
        and n_seq >= 4
        and columns % 128 == 0
        and tokens % 128 == 0
        and sub % 16 == 0
        and half % 16 == 0
        and held < VMEM_BUDGET - 8 * 2**20
    )


def on_device(queries, keys, values, block_order, wo, resid, gain, w_gate, w_up, w_down):
    seq_dev = queries.shape[0]
    heads_dev = queries.shape[1] // HEAD_DIM
    groups = lax.axis_size("section") * lax.axis_size("rep")
    n_seq = lax.axis_size("seq")
    sub_rows = seq_dev // groups
    block_rows = seq_dev // 2
    query_start = lax.axis_index("seq") * seq_dev
    query_pos = key_positions(block_order, query_start, seq_dev, block_rows)
    if kernels_fit(queries, wo, w_gate):
        block = resid.reshape(wo.shape[1], n_seq * sub_rows)
        mixed = layer(block_order, queries, keys, values, wo, block, gain, w_gate, w_up, w_down)
        return mixed.reshape(resid.shape)
    query_heads = queries.reshape(seq_dev, heads_dev, HEAD_DIM)
    scale = HEAD_DIM ** (-0.5)
    running_max = jnp.full((seq_dev, heads_dev), -1e30, jnp.float32)
    key_piece = lax.all_gather(keys, "seq", axis=0, tiled=True)
    value_piece = lax.all_gather(values, "seq", axis=0, tiled=True)
    count = key_piece.shape[0]
    key_pos = key_positions(block_order, jnp.int32(0), count, block_rows)
    scores = (
        jnp.einsum(
            "qhd,khd->qhk",
            query_heads,
            key_piece.reshape(count, heads_dev, HEAD_DIM),
            preferred_element_type=jnp.float32,
        )
        * scale
    )
    visible = (key_pos[None, :] <= query_pos[:, None])[:, None, :]
    new_max = jnp.maximum(running_max, jnp.max(jnp.where(visible, scores, -1e30), axis=-1))
    probs = jnp.where(visible, jnp.exp(scores - new_max[..., None]), 0.0)
    total = jnp.sum(probs, axis=-1)
    weighted = jnp.einsum(
        "qhk,khd->qhd",
        probs.astype(jnp.bfloat16),
        value_piece.reshape(count, heads_dev, HEAD_DIM),
        preferred_element_type=jnp.float32,
    )
    running_max, total, weighted = (new_max, total, weighted)
    attended = (
        (weighted / total[..., None]).astype(jnp.bfloat16).reshape(seq_dev, heads_dev * HEAD_DIM)
    )
    columns = wo.shape[1]
    token_count = n_seq * sub_rows
    parts = attended.reshape(groups, sub_rows, heads_dev * HEAD_DIM)
    group_rows = lax.all_to_all(parts, ("section", "rep"), split_axis=0, concat_axis=2, tiled=True)
    wo_columns = lax.all_gather(wo, ("section", "rep"), axis=0, tiled=True)
    piece = lax.all_gather(group_rows, "seq", axis=0, tiled=True)
    flat = piece.reshape(piece.shape[0] * piece.shape[1], piece.shape[2])
    product = jnp.dot(flat, wo_columns, preferred_element_type=jnp.float32)
    projected = product.reshape(piece.shape[0], piece.shape[1], columns)
    projected_cols = projected.reshape(token_count, columns).T
    carried = resid.reshape(columns, token_count).astype(jnp.float32) + projected_cols
    squares = lax.psum(jnp.sum(carried * carried, axis=0), "seq")
    normed = (
        carried * lax.rsqrt(squares / D + 1e-05)[None, :] * gain.astype(jnp.float32)[:, None]
    ).astype(jnp.bfloat16)
    piece = lax.all_gather(normed, "seq", axis=0, tiled=True)
    gate_sum = jnp.dot(w_gate, piece, preferred_element_type=jnp.float32)
    up_sum = jnp.dot(w_up, piece, preferred_element_type=jnp.float32)
    hidden = (jax.nn.silu(gate_sum) * up_sum).astype(jnp.bfloat16)
    term = lax.dot_general(
        w_down, hidden, (((0,), (0,)), ((), ())), preferred_element_type=jnp.float32
    )
    down = lax.psum_scatter(term, "seq", scatter_dimension=0, tiled=True)
    return (carried + down).astype(jnp.bfloat16).reshape(resid.shape)


def solution(mesh):
    return jax.shard_map(
        on_device,
        mesh=mesh,
        in_specs=(
            P("seq", ("section", "rep")),
            P("seq", ("section", "rep")),
            P("seq", ("section", "rep")),
            P(),
            P(("section", "rep"), "seq"),
            P(("section", "rep"), "seq", None),
            P("seq"),
            P("seq", None),
            P("seq", None),
            P("seq", None),
        ),
        out_specs=P(("section", "rep"), "seq", None),
        check_vma=False,
    )
```

```python
import functools

import jax
import jax.numpy as jnp
from jax import lax
from jax.experimental import pallas as pl
from jax.experimental.pallas import tpu as pltpu
from jax.sharding import PartitionSpec as P

D = 5120
HEAD_DIM = 128


def key_positions(order, start, count, block_rows):
    row_ids = start + jnp.arange(count, dtype=jnp.int32)
    owners = row_ids // block_rows
    match = owners[:, None] == jnp.arange(order.shape[0], dtype=jnp.int32)[None, :]
    first = jnp.sum(jnp.where(match, order[None, :], 0), axis=1)
    return first * block_rows + row_ids % block_rows


VMEM_BUDGET = 60 * 2**20
PIECES = 2


class Copies:
    def __init__(self, send_sems):
        self.sems = send_sems
        self.started = []

    def send(self, src, dst, recv_sem, device, when=None):
        copy = pltpu.make_async_remote_copy(
            src_ref=src,
            dst_ref=dst,
            send_sem=self.sems.at[len(self.started)],
            recv_sem=recv_sem,
            device_id=device,
            device_id_type=pl.DeviceIdType.MESH,
        )
        if when is None:
            copy.start()
        else:
            pl.when(when)(copy.start)
        self.started.append((copy, when))

    def arrived(self, dst, recv_sem, device):
        pltpu.make_async_remote_copy(
            src_ref=dst,
            dst_ref=dst,
            send_sem=self.sems.at[0],
            recv_sem=recv_sem,
            device_id=device,
            device_id_type=pl.DeviceIdType.MESH,
        ).wait_recv()

    def finish(self):
        for copy, when in self.started:
            if when is None:
                copy.wait_send()
            else:
                pl.when(when)(copy.wait_send)


def greet(peers):
    barrier = pltpu.get_barrier_semaphore()
    for peer in peers:
        pl.semaphore_signal(barrier, inc=1, device_id=peer, device_id_type=pl.DeviceIdType.MESH)
    pl.semaphore_wait(barrier, len(peers))


def mask_bias(order_ref, s, rows, count, block_rows):
    row = lax.broadcasted_iota(jnp.int32, (rows, count), 0)
    column = lax.broadcasted_iota(jnp.int32, (1, count), 1)
    second = row >= block_rows
    row_pos = jnp.where(second, order_ref[2 * s + 1], order_ref[2 * s]) * block_rows
    row_pos += jnp.where(second, row - block_rows, row)
    column_pos = jnp.zeros((1, count), jnp.int32)
    for b in range(count // block_rows):
        column_pos = jnp.where(column >= b * block_rows, (order_ref[b] - b) * block_rows + column, column_pos)
    return jnp.where(column_pos <= row_pos, 0.0, -1e30).astype(jnp.float32)


def layer_kernel(
    n_seq, n_rep, groups,
    order_ref, q_ref, k_ref, v_ref, wo_ref, resid_ref, gain_ref, w_gate_hbm, w_up_hbm, w_down_hbm, out_ref,
    keys, values, attended, bias, proj, proj_low, from_group, carried,
    x, sq, w_gate, w_up, w_down, gate_acc, up_acc, hidden, part, from_rep, to_y, from_y, to_z, from_z,
    weight_sem, own_sem, send_sem, k_sem, v_sem, att_sem, group_sem, x_sem, sq_sem, rep_sem, y_sem, z_sem,
):
    section, s, r = lax.axis_index("section"), lax.axis_index("seq"), lax.axis_index("rep")
    depth = n_seq // 2
    columns, tokens = resid_ref.shape
    seq_dev = q_ref.shape[0]
    block_rows = seq_dev // 2
    sub = seq_dev // groups
    half = w_gate.shape[0]
    z, y = s // 2, lax.rem(s, 2)
    other_y, other_r = 1 - y, 1 - r
    group = section * n_rep + r

    def at(z_step, y_index):
        return lax.rem(z + z_step, depth) * 2 + y_index

    def dev(seq_index, rep_index):
        return (section, seq_index, rep_index)

    def nearest(step):
        near = z + (step + 1) // 2 * (1 if step % 2 == 0 else -1)
        far = jnp.where(2 * z < depth - 1, step, depth - 1 - step)
        return jnp.where(step <= 2 * jnp.minimum(z, depth - 1 - z), near, far)

    sources = [z] + [nearest(step) for step in range(1, depth)]
    above, below = jnp.minimum(z + 1, depth - 1), jnp.maximum(z - 1, 0)

    def group_dev(step):
        other = lax.rem(group + step, groups)
        return (other // n_rep, s, lax.rem(other, n_rep))

    rep_mate, y_mate = dev(s, other_r), dev(at(0, other_y), r)
    loads = []
    for i, (hbm, vmem) in enumerate(((w_gate_hbm, w_gate), (w_up_hbm, w_up), (w_down_hbm, w_down))):
        load = pltpu.make_async_copy(hbm.at[pl.ds(r * half, half), :], vmem, weight_sem.at[i])
        load.start()
        loads.append(load)

    def rows(rep_index):
        return pl.ds(rep_index * tokens, tokens)

    own = [
        pltpu.make_async_copy(k_ref, keys.at[s], own_sem.at[0]),
        pltpu.make_async_copy(v_ref, values.at[s], own_sem.at[1]),
    ]
    for copy in own:
        copy.start()
    peers = [
        dev(lax.rem(s + k, n_seq), rep_index)
        for k in range(n_seq)
        for rep_index in (r, other_r)
        if (k, rep_index is r) != (0, True)
    ]
    greet(peers + [(lax.rem(section + k, groups // n_rep), s, i) for k in range(1, groups // n_rep) for i in range(n_rep)])
    copies = Copies(send_sem)

    def along(src, dst, sem):
        copies.send(src, dst, sem, dev(above * 2 + y, r), when=z < depth - 1)
        copies.send(src, dst, sem, dev(below * 2 + y, r), when=z > 0)

    def onward(piece, sem, source):
        up = source < z
        device = dev(jnp.where(up, above, below) * 2 + y, r)
        more = jnp.where(up, z < depth - 1, z > 0)
        copies.send(piece, piece, sem, device, when=more)

    seq_rows = seq_dev // PIECES

    def spread(src, dst, sem):
        for p in range(PIECES):
            span = pl.ds(p * seq_rows, seq_rows)
            along(src.at[span, :], dst.at[s, span, :], sem.at[s, p])
            copies.send(src.at[span, :], dst.at[s, span, :], sem.at[s, p], y_mate)

    def take(dst, sem, k, from_mate):
        seq_index = sources[k] * 2 + (other_y if from_mate else y)
        for p in range(PIECES):
            piece = dst.at[seq_index, pl.ds(p * seq_rows, seq_rows), :]
            copies.arrived(piece, sem.at[seq_index, p], y_mate)
            if not from_mate:
                onward(piece, sem.at[seq_index, p], sources[k])
                copies.send(piece, piece, sem.at[seq_index, p], y_mate)
        return seq_index

    events = []
    for k in range(depth):
        if k:
            events.append((k, 0))
            events.append((k - 1, 1))
    events.append((depth - 1, 1))

    spread(k_ref, keys, k_sem)
    spread(v_ref, values, v_sem)
    for k in range(1, depth):
        take(keys, k_sem, k, 0)
        take(values, v_sem, k, 0)
        if k == 1:
            carried[...] = jnp.transpose(resid_ref[...].astype(jnp.float32))
            bias[...] = mask_bias(order_ref, s, seq_dev, n_seq * seq_dev, block_rows)
    for copy in own:
        copy.wait()
    for k in range(depth):
        take(keys, k_sem, k, 1)
    heads = q_ref.shape[1] // HEAD_DIM
    all_keys = keys.reshape(n_seq * seq_dev, q_ref.shape[1])
    all_values = values.reshape(n_seq * seq_dev, q_ref.shape[1])
    probs, totals = [], []
    for h in range(heads):
        span = slice(h * HEAD_DIM, (h + 1) * HEAD_DIM)
        scores = lax.dot_general(
            q_ref[:, span], all_keys[:, span], (((1,), (1,)), ((), ())), preferred_element_type=jnp.float32
        )
        scores = scores * HEAD_DIM**-0.5 + bias[...]
        prob = jnp.exp(scores - jnp.max(scores, axis=1, keepdims=True))
        totals.append(jnp.sum(prob, axis=1, keepdims=True))
        probs.append(prob.astype(jnp.bfloat16))
    for k in range(depth):
        take(values, v_sem, k, 1)
    for h in range(heads):
        span = slice(h * HEAD_DIM, (h + 1) * HEAD_DIM)
        weighted = jnp.dot(probs[h], all_values[:, span], preferred_element_type=jnp.float32)
        attended[s, :, span] = (weighted / totals[h]).astype(jnp.bfloat16)
    spread(attended.at[s], attended, att_sem)

    def project(seq_index):
        proj[...] = jnp.dot(attended[seq_index], wo_ref[...], preferred_element_type=jnp.float32)
        proj_low[seq_index] = proj[...].astype(jnp.bfloat16)
        spot = pl.ds(pl.multiple_of(seq_index * sub, sub), sub)
        carried[spot, :] += proj[pl.ds(pl.multiple_of(group * sub, sub), sub), :]
        for step in range(1, groups):
            other = lax.rem(group + step, groups)
            copies.send(
                proj_low.at[seq_index, pl.ds(pl.multiple_of(other * sub, sub), sub), :],
                from_group.at[step - 1, spot, :],
                group_sem.at[step - 1, seq_index],
                group_dev(step),
            )

    pending = s
    for k, from_mate in events:
        seq_index = take(attended, att_sem, k, from_mate)
        project(pending)
        pending = seq_index
    project(pending)
    for step in range(1, groups):
        for k in range(n_seq):
            spot = pl.ds(k * sub, sub)
            copies.arrived(from_group.at[step - 1, spot, :], group_sem.at[step - 1, k], rep_mate)
    total = carried[...]
    for step in range(1, groups):
        total += from_group[step - 1].astype(jnp.float32)
    carried[...] = total
    squares = jnp.sum(total * total, axis=1, keepdims=True)
    sq[s, r] = jnp.transpose(jnp.broadcast_to(squares, (tokens, tokens)))[:8]
    x[s, rows(r), :] = (total * gain_ref[...].astype(jnp.float32).reshape(1, columns)).astype(jnp.bfloat16)
    piece_rows = tokens // PIECES

    def piece_of(seq_index, rep_index, p):
        return x.at[seq_index, pl.ds(rep_index * tokens + p * piece_rows, piece_rows), :]

    def forward(seq_index, p, device):
        piece = piece_of(seq_index, r, p)
        copies.send(piece, piece, x_sem.at[seq_index, r, p], device)

    for p in range(PIECES):
        mine = piece_of(s, r, p)
        along(mine, mine, x_sem.at[s, r, p])
        forward(s, p, y_mate)
        forward(s, p, rep_mate)
    for peer in peers:
        copies.send(sq.at[s, r], sq.at[s, r], sq_sem.at[s, r], peer)

    first = True

    def accumulate(seq_index):
        nonlocal first
        for p in range(PIECES):
            copies.arrived(piece_of(seq_index, other_r, p), x_sem.at[seq_index, other_r, p], rep_mate)
        block = x[seq_index]
        span = pl.ds(pl.multiple_of(seq_index * columns, 128), columns)
        for w, acc, load in ((w_gate, gate_acc, loads[0]), (w_up, up_acc, loads[1])):
            if first:
                load.wait()
            term = lax.dot_general(
                block, w[:, span], (((1,), (1,)), ((), ())), preferred_element_type=jnp.float32
            )
            if first:
                acc[...] = term
            else:
                acc[...] += term
        first = False

    pending = s
    for k, from_mate in events:
        seq_index = sources[k] * 2 + (other_y if from_mate else y)
        for p in range(PIECES):
            piece = piece_of(seq_index, r, p)
            copies.arrived(piece, x_sem.at[seq_index, r, p], y_mate)
            if not from_mate:
                onward(piece, x_sem.at[seq_index, r, p], sources[k])
                forward(seq_index, p, y_mate)
            forward(seq_index, p, rep_mate)
        accumulate(pending)
        pending = seq_index
    for k in range(n_seq):
        for rep_index in (r, other_r):
            if (k, rep_index is r) != (0, True):
                seq_index = lax.rem(s + k, n_seq)
                copies.arrived(sq.at[seq_index, rep_index], sq_sem.at[seq_index, rep_index], rep_mate)
    accumulate(pending)

    for rep_index in range(2):
        total = jnp.sum(sq[:, rep_index], axis=0)
        factor = lax.rsqrt(total / (n_seq * columns) + 1e-05)
        factor = jnp.transpose(factor)[:, :1]
        own_rows = slice(rep_index * tokens, (rep_index + 1) * tokens)
        gate = gate_acc[own_rows, :] * factor
        up = up_acc[own_rows, :] * factor
        hidden[own_rows, :] = (gate / (1.0 + jnp.exp(-gate)) * up).astype(jnp.bfloat16)
    loads[2].wait()

    order = [(k % depth, 1) for k in range(1, depth + 1)] + [(k % depth, 0) for k in range(1, depth + 1)]
    slot_of = {step: i for i, step in enumerate(order)}

    def joined(slot):
        return part[slot, rows(r), :] + from_rep[slot]

    def after_rep(slot):
        k, to_mate = order[slot]
        copies.arrived(from_rep.at[slot], rep_sem.at[slot], rep_mate)
        if to_mate:
            to_y[k] = joined(slot).astype(jnp.bfloat16)
            copies.send(to_y.at[k], from_y.at[k], y_sem.at[k], y_mate)

    for slot, (k, to_mate) in enumerate(order):
        seq_index = at(k, other_y if to_mate else y)
        span = pl.ds(pl.multiple_of(seq_index * columns, 128), columns)
        part[slot] = jnp.dot(hidden[...], w_down[:, span], preferred_element_type=jnp.float32)
        copies.send(part.at[slot, rows(other_r), :], from_rep.at[slot], rep_sem.at[slot], rep_mate)
        if slot:
            after_rep(slot - 1)
    after_rep(len(order) - 1)
    for k in range(1, depth):
        copies.arrived(from_y.at[k], y_sem.at[k], y_mate)
        to_z[k - 1] = (joined(slot_of[k, 0]) + from_y[k].astype(jnp.float32)).astype(jnp.bfloat16)
        copies.send(to_z.at[k - 1], from_z.at[k - 1], z_sem.at[k - 1], dev(at(k, y), r))
    copies.arrived(from_y.at[0], y_sem.at[0], y_mate)
    total = carried[...] + joined(slot_of[0, 0]) + from_y[0].astype(jnp.float32)
    for k in range(1, depth):
        copies.arrived(from_z.at[k - 1], z_sem.at[k - 1], y_mate)
        total += from_z[k - 1].astype(jnp.float32)
    out_ref[...] = jnp.transpose(total).astype(jnp.bfloat16)
    copies.finish()


def layer(order, q, k, v, wo, resid, gain, w_gate, w_up, w_down):
    n_seq, n_rep = lax.axis_size("seq"), lax.axis_size("rep")
    groups = n_rep * lax.axis_size("section")
    seq_dev, width = q.shape
    columns, tokens = resid.shape
    features = w_gate.shape[1]
    half = w_gate.shape[0] // n_rep
    depth = n_seq // 2
    blocks = PIECES * (3 * (1 + n_seq) + 4 + 2 * (depth - 1) + n_seq - 1)
    sends = blocks + n_seq * (groups - 1) + (n_rep * n_seq - 1) + n_seq + 2 * depth - 1
    f32, bf16 = jnp.float32, jnp.bfloat16
    vmem = pl.BlockSpec(memory_space=pltpu.VMEM)
    hbm = pl.BlockSpec(memory_space=pl.ANY)
    dma = pltpu.SemaphoreType.DMA
    return pl.pallas_call(
        functools.partial(layer_kernel, n_seq, n_rep, groups),
        out_shape=jax.ShapeDtypeStruct((columns, tokens), bf16),
        in_specs=[pl.BlockSpec(memory_space=pltpu.SMEM)] + [vmem] * 6 + [hbm] * 3,
        out_specs=vmem,
        scratch_shapes=[
            pltpu.VMEM((n_seq, seq_dev, width), bf16),
            pltpu.VMEM((n_seq, seq_dev, width), bf16),
            pltpu.VMEM((n_seq, seq_dev, width), bf16),
            pltpu.VMEM((seq_dev, n_seq * seq_dev), f32),
            pltpu.VMEM((seq_dev, columns), f32),
            pltpu.VMEM((n_seq, seq_dev, columns), bf16),
            pltpu.VMEM((groups - 1, tokens, columns), bf16),
            pltpu.VMEM((tokens, columns), f32),
            pltpu.VMEM((n_seq, n_rep * tokens, columns), bf16),
            pltpu.VMEM((n_seq, n_rep, 8, tokens), f32),
            pltpu.VMEM((half, features), bf16),
            pltpu.VMEM((half, features), bf16),
            pltpu.VMEM((half, features), bf16),
            pltpu.VMEM((n_rep * tokens, half), f32),
            pltpu.VMEM((n_rep * tokens, half), f32),
            pltpu.VMEM((n_rep * tokens, half), bf16),
            pltpu.VMEM((n_seq, n_rep * tokens, columns), f32),
            pltpu.VMEM((n_seq, tokens, columns), f32),
            pltpu.VMEM((depth, tokens, columns), bf16),
            pltpu.VMEM((depth, tokens, columns), bf16),
            pltpu.VMEM((depth - 1, tokens, columns), bf16),
            pltpu.VMEM((depth - 1, tokens, columns), bf16),
            dma((3,)),
            dma((2,)),
            dma((sends,)),
            dma((n_seq, PIECES)),
            dma((n_seq, PIECES)),
            dma((n_seq, PIECES)),
            dma((groups - 1, n_seq)),
            dma((n_seq, n_rep, PIECES)),
            dma((n_seq, n_rep)),
            dma((n_seq,)),
            dma((depth,)),
            dma((depth - 1,)),
        ],
        compiler_params=pltpu.CompilerParams(
            collective_id=1, has_side_effects=True, vmem_limit_bytes=VMEM_BUDGET
        ),
    )(order, q, k, v, wo, resid, gain, w_gate, w_up, w_down)


def kernels_fit(queries, wo, w_gate):
    n_seq, n_rep = lax.axis_size("seq"), lax.axis_size("rep")
    columns = wo.shape[1]
    sub = queries.shape[0] // (n_rep * lax.axis_size("section"))
    tokens = n_seq * sub
    half = w_gate.shape[0] // n_rep
    held = 3 * half * w_gate.shape[1] * 2 + n_seq * tokens * columns * 18 + 20 * tokens * half
    return (
        n_rep == 2
        and n_seq % 2 == 0
        and n_seq >= 4
        and columns % 128 == 0
        and tokens % 128 == 0
        and sub % 16 == 0
        and queries.shape[0] % (16 * PIECES) == 0
        and half % 16 == 0
        and held < VMEM_BUDGET - 8 * 2**20
    )


def on_device(queries, keys, values, block_order, wo, resid, gain, w_gate, w_up, w_down):
    seq_dev = queries.shape[0]
    heads_dev = queries.shape[1] // HEAD_DIM
    groups = lax.axis_size("section") * lax.axis_size("rep")
    n_seq = lax.axis_size("seq")
    sub_rows = seq_dev // groups
    block_rows = seq_dev // 2
    query_start = lax.axis_index("seq") * seq_dev
    query_pos = key_positions(block_order, query_start, seq_dev, block_rows)
    if kernels_fit(queries, wo, w_gate):
        block = resid.reshape(wo.shape[1], n_seq * sub_rows)
        mixed = layer(block_order, queries, keys, values, wo, block, gain, w_gate, w_up, w_down)
        return mixed.reshape(resid.shape)
    query_heads = queries.reshape(seq_dev, heads_dev, HEAD_DIM)
    scale = HEAD_DIM ** (-0.5)
    running_max = jnp.full((seq_dev, heads_dev), -1e30, jnp.float32)
    key_piece = lax.all_gather(keys, "seq", axis=0, tiled=True)
    value_piece = lax.all_gather(values, "seq", axis=0, tiled=True)
    count = key_piece.shape[0]
    key_pos = key_positions(block_order, jnp.int32(0), count, block_rows)
    scores = (
        jnp.einsum(
            "qhd,khd->qhk",
            query_heads,
            key_piece.reshape(count, heads_dev, HEAD_DIM),
            preferred_element_type=jnp.float32,
        )
        * scale
    )
    visible = (key_pos[None, :] <= query_pos[:, None])[:, None, :]
    new_max = jnp.maximum(running_max, jnp.max(jnp.where(visible, scores, -1e30), axis=-1))
    probs = jnp.where(visible, jnp.exp(scores - new_max[..., None]), 0.0)
    total = jnp.sum(probs, axis=-1)
    weighted = jnp.einsum(
        "qhk,khd->qhd",
        probs.astype(jnp.bfloat16),
        value_piece.reshape(count, heads_dev, HEAD_DIM),
        preferred_element_type=jnp.float32,
    )
    running_max, total, weighted = (new_max, total, weighted)
    attended = (
        (weighted / total[..., None]).astype(jnp.bfloat16).reshape(seq_dev, heads_dev * HEAD_DIM)
    )
    columns = wo.shape[1]
    token_count = n_seq * sub_rows
    parts = attended.reshape(groups, sub_rows, heads_dev * HEAD_DIM)
    group_rows = lax.all_to_all(parts, ("section", "rep"), split_axis=0, concat_axis=2, tiled=True)
    wo_columns = lax.all_gather(wo, ("section", "rep"), axis=0, tiled=True)
    piece = lax.all_gather(group_rows, "seq", axis=0, tiled=True)
    flat = piece.reshape(piece.shape[0] * piece.shape[1], piece.shape[2])
    product = jnp.dot(flat, wo_columns, preferred_element_type=jnp.float32)
    projected = product.reshape(piece.shape[0], piece.shape[1], columns)
    projected_cols = projected.reshape(token_count, columns).T
    carried = resid.reshape(columns, token_count).astype(jnp.float32) + projected_cols
    squares = lax.psum(jnp.sum(carried * carried, axis=0), "seq")
    normed = (
        carried * lax.rsqrt(squares / D + 1e-05)[None, :] * gain.astype(jnp.float32)[:, None]
    ).astype(jnp.bfloat16)
    piece = lax.all_gather(normed, "seq", axis=0, tiled=True)
    gate_sum = jnp.dot(w_gate, piece, preferred_element_type=jnp.float32)
    up_sum = jnp.dot(w_up, piece, preferred_element_type=jnp.float32)
    hidden = (jax.nn.silu(gate_sum) * up_sum).astype(jnp.bfloat16)
    term = lax.dot_general(
        w_down, hidden, (((0,), (0,)), ((), ())), preferred_element_type=jnp.float32
    )
    down = lax.psum_scatter(term, "seq", scatter_dimension=0, tiled=True)
    return (carried + down).astype(jnp.bfloat16).reshape(resid.shape)


def solution(mesh):
    return jax.shard_map(
        on_device,
        mesh=mesh,
        in_specs=(
            P("seq", ("section", "rep")),
            P("seq", ("section", "rep")),
            P("seq", ("section", "rep")),
            P(),
            P(("section", "rep"), "seq"),
            P(("section", "rep"), "seq", None),
            P("seq"),
            P("seq", None),
            P("seq", None),
            P("seq", None),
        ),
        out_specs=P(("section", "rep"), "seq", None),
        check_vma=False,
    )
```

```python
import functools

import jax
import jax.numpy as jnp
from jax import lax
from jax.experimental import pallas as pl
from jax.experimental.pallas import tpu as pltpu
from jax.sharding import PartitionSpec as P

D = 5120
HEAD_DIM = 128


def key_positions(order, start, count, block_rows):
    row_ids = start + jnp.arange(count, dtype=jnp.int32)
    owners = row_ids // block_rows
    match = owners[:, None] == jnp.arange(order.shape[0], dtype=jnp.int32)[None, :]
    first = jnp.sum(jnp.where(match, order[None, :], 0), axis=1)
    return first * block_rows + row_ids % block_rows


VMEM_BUDGET = 60 * 2**20
PIECES = 2


class Copies:
    def __init__(self, send_sems):
        self.sems = send_sems
        self.started = []

    def send(self, src, dst, recv_sem, device, when=None):
        copy = pltpu.make_async_remote_copy(
            src_ref=src,
            dst_ref=dst,
            send_sem=self.sems.at[len(self.started)],
            recv_sem=recv_sem,
            device_id=device,
            device_id_type=pl.DeviceIdType.MESH,
        )
        if when is None:
            copy.start()
        else:
            pl.when(when)(copy.start)
        self.started.append((copy, when))

    def arrived(self, dst, recv_sem, device):
        pltpu.make_async_remote_copy(
            src_ref=dst,
            dst_ref=dst,
            send_sem=self.sems.at[0],
            recv_sem=recv_sem,
            device_id=device,
            device_id_type=pl.DeviceIdType.MESH,
        ).wait_recv()

    def finish(self):
        for copy, when in self.started:
            if when is None:
                copy.wait_send()
            else:
                pl.when(when)(copy.wait_send)


def greet(peers):
    barrier = pltpu.get_barrier_semaphore()
    for peer in peers:
        pl.semaphore_signal(barrier, inc=1, device_id=peer, device_id_type=pl.DeviceIdType.MESH)
    pl.semaphore_wait(barrier, len(peers))


def mask_bias(order_ref, s, rows, count, block_rows):
    row = lax.broadcasted_iota(jnp.int32, (rows, count), 0)
    column = lax.broadcasted_iota(jnp.int32, (1, count), 1)
    second = row >= block_rows
    row_pos = jnp.where(second, order_ref[2 * s + 1], order_ref[2 * s]) * block_rows
    row_pos += jnp.where(second, row - block_rows, row)
    column_pos = jnp.zeros((1, count), jnp.int32)
    for b in range(count // block_rows):
        column_pos = jnp.where(column >= b * block_rows, (order_ref[b] - b) * block_rows + column, column_pos)
    return jnp.where(column_pos <= row_pos, 0.0, -1e30).astype(jnp.float32)


def layer_kernel(
    n_seq, n_rep, groups,
    order_ref, q_ref, k_ref, v_ref, wo_ref, resid_ref, gain_ref, w_gate_hbm, w_up_hbm, w_down_hbm, out_ref,
    keys, values, attended, bias, proj, proj_low, from_group, carried,
    x, sq, w_gate, w_up, w_down, gate_acc, up_acc, hidden, part, from_rep, to_y, from_y, to_z, from_z,
    weight_sem, own_sem, send_sem, k_sem, v_sem, att_sem, group_sem, x_sem, sq_sem, rep_sem, y_sem, z_sem,
):
    section, s, r = lax.axis_index("section"), lax.axis_index("seq"), lax.axis_index("rep")
    depth = n_seq // 2
    columns, tokens = resid_ref.shape
    seq_dev = q_ref.shape[0]
    block_rows = seq_dev // 2
    sub = seq_dev // groups
    half = w_gate.shape[0]
    z, y = s // 2, lax.rem(s, 2)
    other_y, other_r = 1 - y, 1 - r
    group = section * n_rep + r

    def at(z_step, y_index):
        return lax.rem(z + z_step, depth) * 2 + y_index

    def dev(seq_index, rep_index):
        return (section, seq_index, rep_index)

    def nearest(step):
        near = z + (step + 1) // 2 * (1 if step % 2 == 0 else -1)
        far = jnp.where(2 * z < depth - 1, step, depth - 1 - step)
        return jnp.where(step <= 2 * jnp.minimum(z, depth - 1 - z), near, far)

    sources = [z] + [nearest(step) for step in range(1, depth)]
    above, below = jnp.minimum(z + 1, depth - 1), jnp.maximum(z - 1, 0)

    def group_dev(step):
        other = lax.rem(group + step, groups)
        return (other // n_rep, s, lax.rem(other, n_rep))

    rep_mate, y_mate = dev(s, other_r), dev(at(0, other_y), r)
    loads = []
    for i, (hbm, vmem) in enumerate(((w_gate_hbm, w_gate), (w_up_hbm, w_up), (w_down_hbm, w_down))):
        load = pltpu.make_async_copy(hbm.at[pl.ds(r * half, half), :], vmem, weight_sem.at[i])
        load.start()
        loads.append(load)

    def rows(rep_index):
        return pl.ds(rep_index * tokens, tokens)

    own = [
        pltpu.make_async_copy(k_ref, keys.at[s], own_sem.at[0]),
        pltpu.make_async_copy(v_ref, values.at[s], own_sem.at[1]),
    ]
    for copy in own:
        copy.start()
    peers = [
        dev(lax.rem(s + k, n_seq), rep_index)
        for k in range(n_seq)
        for rep_index in (r, other_r)
        if (k, rep_index is r) != (0, True)
    ]
    greet(peers + [(lax.rem(section + k, groups // n_rep), s, i) for k in range(1, groups // n_rep) for i in range(n_rep)])
    copies = Copies(send_sem)

    def along(src, dst, sem):
        copies.send(src, dst, sem, dev(above * 2 + y, r), when=z < depth - 1)
        copies.send(src, dst, sem, dev(below * 2 + y, r), when=z > 0)

    def onward(piece, sem, source):
        up = source < z
        device = dev(jnp.where(up, above, below) * 2 + y, r)
        more = jnp.where(up, z < depth - 1, z > 0)
        copies.send(piece, piece, sem, device, when=more)

    seq_rows = seq_dev // PIECES

    def spread(src, dst, sem):
        for p in range(PIECES):
            span = pl.ds(p * seq_rows, seq_rows)
            along(src.at[span, :], dst.at[s, span, :], sem.at[s, p])
            copies.send(src.at[span, :], dst.at[s, span, :], sem.at[s, p], y_mate)

    def take(dst, sem, k, from_mate):
        seq_index = sources[k] * 2 + (other_y if from_mate else y)
        for p in range(PIECES):
            piece = dst.at[seq_index, pl.ds(p * seq_rows, seq_rows), :]
            copies.arrived(piece, sem.at[seq_index, p], y_mate)
            if not from_mate:
                onward(piece, sem.at[seq_index, p], sources[k])
                copies.send(piece, piece, sem.at[seq_index, p], y_mate)
        return seq_index

    events = []
    for k in range(depth):
        if k:
            events.append((k, 0))
            events.append((k - 1, 1))
    events.append((depth - 1, 1))

    spread(k_ref, keys, k_sem)
    spread(v_ref, values, v_sem)
    for k in range(1, depth):
        take(keys, k_sem, k, 0)
        take(values, v_sem, k, 0)
        if k == 1:
            carried[...] = jnp.transpose(resid_ref[...].astype(jnp.float32))
            bias[...] = mask_bias(order_ref, s, seq_dev, n_seq * seq_dev, block_rows)
    for copy in own:
        copy.wait()
    for k in range(depth):
        take(keys, k_sem, k, 1)
    heads = q_ref.shape[1] // HEAD_DIM
    all_keys = keys.reshape(n_seq * seq_dev, q_ref.shape[1])
    all_values = values.reshape(n_seq * seq_dev, q_ref.shape[1])
    probs, totals = [], []
    for h in range(heads):
        span = slice(h * HEAD_DIM, (h + 1) * HEAD_DIM)
        scores = lax.dot_general(
            q_ref[:, span], all_keys[:, span], (((1,), (1,)), ((), ())), preferred_element_type=jnp.float32
        )
        scores = scores * HEAD_DIM**-0.5 + bias[...]
        prob = jnp.exp(scores - jnp.max(scores, axis=1, keepdims=True))
        totals.append(jnp.sum(prob, axis=1, keepdims=True))
        probs.append(prob.astype(jnp.bfloat16))
    for k in range(depth):
        take(values, v_sem, k, 1)
    for h in range(heads):
        span = slice(h * HEAD_DIM, (h + 1) * HEAD_DIM)
        weighted = jnp.dot(probs[h], all_values[:, span], preferred_element_type=jnp.float32)
        attended[s, :, span] = (weighted / totals[h]).astype(jnp.bfloat16)
    spread(attended.at[s], attended, att_sem)

    def project(seq_index):
        proj[...] = jnp.dot(attended[seq_index], wo_ref[...], preferred_element_type=jnp.float32)
        proj_low[seq_index] = proj[...].astype(jnp.bfloat16)
        spot = pl.ds(pl.multiple_of(seq_index * sub, sub), sub)
        carried[spot, :] += proj[pl.ds(pl.multiple_of(group * sub, sub), sub), :]
        for step in range(1, groups):
            other = lax.rem(group + step, groups)
            copies.send(
                proj_low.at[seq_index, pl.ds(pl.multiple_of(other * sub, sub), sub), :],
                from_group.at[step - 1, spot, :],
                group_sem.at[step - 1, seq_index],
                group_dev(step),
            )

    pending = s
    for k, from_mate in events:
        seq_index = take(attended, att_sem, k, from_mate)
        project(pending)
        pending = seq_index
    project(pending)
    for step in range(1, groups):
        for k in range(n_seq):
            spot = pl.ds(k * sub, sub)
            copies.arrived(from_group.at[step - 1, spot, :], group_sem.at[step - 1, k], rep_mate)
    total = carried[...]
    for step in range(1, groups):
        total += from_group[step - 1].astype(jnp.float32)
    carried[...] = total
    squares = jnp.sum(total * total, axis=1, keepdims=True)
    sq[s, r] = jnp.transpose(jnp.broadcast_to(squares, (tokens, tokens)))[:8]
    x[s, rows(r), :] = (total * gain_ref[...].astype(jnp.float32).reshape(1, columns)).astype(jnp.bfloat16)
    piece_rows = tokens // PIECES

    def piece_of(seq_index, rep_index, p):
        return x.at[seq_index, pl.ds(rep_index * tokens + p * piece_rows, piece_rows), :]

    def forward(seq_index, p, device):
        piece = piece_of(seq_index, r, p)
        copies.send(piece, piece, x_sem.at[seq_index, r, p], device)

    for p in range(PIECES):
        mine = piece_of(s, r, p)
        along(mine, mine, x_sem.at[s, r, p])
        forward(s, p, y_mate)
        forward(s, p, rep_mate)
    for peer in peers:
        copies.send(sq.at[s, r], sq.at[s, r], sq_sem.at[s, r], peer)

    first = True

    def accumulate(seq_index):
        nonlocal first
        for p in range(PIECES):
            copies.arrived(piece_of(seq_index, other_r, p), x_sem.at[seq_index, other_r, p], rep_mate)
        block = x[seq_index]
        span = pl.ds(pl.multiple_of(seq_index * columns, 128), columns)
        for w, acc, load in ((w_gate, gate_acc, loads[0]), (w_up, up_acc, loads[1])):
            if first:
                load.wait()
            term = lax.dot_general(
                w[:, span], block, (((1,), (1,)), ((), ())), preferred_element_type=jnp.float32
            )
            if first:
                acc[...] = term
            else:
                acc[...] += term
        first = False

    pending = s
    for k, from_mate in events:
        seq_index = sources[k] * 2 + (other_y if from_mate else y)
        for p in range(PIECES):
            piece = piece_of(seq_index, r, p)
            copies.arrived(piece, x_sem.at[seq_index, r, p], y_mate)
            if not from_mate:
                onward(piece, x_sem.at[seq_index, r, p], sources[k])
                forward(seq_index, p, y_mate)
            forward(seq_index, p, rep_mate)
        accumulate(pending)
        pending = seq_index
    for k in range(n_seq):
        for rep_index in (r, other_r):
            if (k, rep_index is r) != (0, True):
                seq_index = lax.rem(s + k, n_seq)
                copies.arrived(sq.at[seq_index, rep_index], sq_sem.at[seq_index, rep_index], rep_mate)
    accumulate(pending)

    for rep_index in range(2):
        total = jnp.sum(sq[:, rep_index], axis=0)
        factor = lax.rsqrt(total / (n_seq * columns) + 1e-05)[:1]
        span = slice(rep_index * tokens, (rep_index + 1) * tokens)
        gate = gate_acc[:, span] * factor
        up = up_acc[:, span] * factor
        hidden[span, :] = jnp.transpose(gate / (1.0 + jnp.exp(-gate)) * up).astype(jnp.bfloat16)
    loads[2].wait()

    order = [(k % depth, 1) for k in range(1, depth + 1)] + [(k % depth, 0) for k in range(1, depth + 1)]
    slot_of = {step: i for i, step in enumerate(order)}

    def joined(slot):
        return part[slot, rows(r), :] + from_rep[slot]

    def after_rep(slot):
        k, to_mate = order[slot]
        copies.arrived(from_rep.at[slot], rep_sem.at[slot], rep_mate)
        if to_mate:
            to_y[k] = joined(slot).astype(jnp.bfloat16)
            copies.send(to_y.at[k], from_y.at[k], y_sem.at[k], y_mate)

    for slot, (k, to_mate) in enumerate(order):
        seq_index = at(k, other_y if to_mate else y)
        span = pl.ds(pl.multiple_of(seq_index * columns, 128), columns)
        part[slot] = jnp.dot(hidden[...], w_down[:, span], preferred_element_type=jnp.float32)
        copies.send(part.at[slot, rows(other_r), :], from_rep.at[slot], rep_sem.at[slot], rep_mate)
        if slot:
            after_rep(slot - 1)
    after_rep(len(order) - 1)
    for k in range(1, depth):
        copies.arrived(from_y.at[k], y_sem.at[k], y_mate)
        to_z[k - 1] = (joined(slot_of[k, 0]) + from_y[k].astype(jnp.float32)).astype(jnp.bfloat16)
        copies.send(to_z.at[k - 1], from_z.at[k - 1], z_sem.at[k - 1], dev(at(k, y), r))
    copies.arrived(from_y.at[0], y_sem.at[0], y_mate)
    total = carried[...] + joined(slot_of[0, 0]) + from_y[0].astype(jnp.float32)
    for k in range(1, depth):
        copies.arrived(from_z.at[k - 1], z_sem.at[k - 1], y_mate)
        total += from_z[k - 1].astype(jnp.float32)
    out_ref[...] = jnp.transpose(total).astype(jnp.bfloat16)
    copies.finish()


def layer(order, q, k, v, wo, resid, gain, w_gate, w_up, w_down):
    n_seq, n_rep = lax.axis_size("seq"), lax.axis_size("rep")
    groups = n_rep * lax.axis_size("section")
    seq_dev, width = q.shape
    columns, tokens = resid.shape
    features = w_gate.shape[1]
    half = w_gate.shape[0] // n_rep
    depth = n_seq // 2
    blocks = PIECES * (3 * (1 + n_seq) + 4 + 2 * (depth - 1) + n_seq - 1)
    sends = blocks + n_seq * (groups - 1) + (n_rep * n_seq - 1) + n_seq + 2 * depth - 1
    f32, bf16 = jnp.float32, jnp.bfloat16
    vmem = pl.BlockSpec(memory_space=pltpu.VMEM)
    hbm = pl.BlockSpec(memory_space=pl.ANY)
    dma = pltpu.SemaphoreType.DMA
    return pl.pallas_call(
        functools.partial(layer_kernel, n_seq, n_rep, groups),
        out_shape=jax.ShapeDtypeStruct((columns, tokens), bf16),
        in_specs=[pl.BlockSpec(memory_space=pltpu.SMEM)] + [vmem] * 6 + [hbm] * 3,
        out_specs=vmem,
        scratch_shapes=[
            pltpu.VMEM((n_seq, seq_dev, width), bf16),
            pltpu.VMEM((n_seq, seq_dev, width), bf16),
            pltpu.VMEM((n_seq, seq_dev, width), bf16),
            pltpu.VMEM((seq_dev, n_seq * seq_dev), f32),
            pltpu.VMEM((seq_dev, columns), f32),
            pltpu.VMEM((n_seq, seq_dev, columns), bf16),
            pltpu.VMEM((groups - 1, tokens, columns), bf16),
            pltpu.VMEM((tokens, columns), f32),
            pltpu.VMEM((n_seq, n_rep * tokens, columns), bf16),
            pltpu.VMEM((n_seq, n_rep, 8, tokens), f32),
            pltpu.VMEM((half, features), bf16),
            pltpu.VMEM((half, features), bf16),
            pltpu.VMEM((half, features), bf16),
            pltpu.VMEM((half, n_rep * tokens), f32),
            pltpu.VMEM((half, n_rep * tokens), f32),
            pltpu.VMEM((n_rep * tokens, half), bf16),
            pltpu.VMEM((n_seq, n_rep * tokens, columns), f32),
            pltpu.VMEM((n_seq, tokens, columns), f32),
            pltpu.VMEM((depth, tokens, columns), bf16),
            pltpu.VMEM((depth, tokens, columns), bf16),
            pltpu.VMEM((depth - 1, tokens, columns), bf16),
            pltpu.VMEM((depth - 1, tokens, columns), bf16),
            dma((3,)),
            dma((2,)),
            dma((sends,)),
            dma((n_seq, PIECES)),
            dma((n_seq, PIECES)),
            dma((n_seq, PIECES)),
            dma((groups - 1, n_seq)),
            dma((n_seq, n_rep, PIECES)),
            dma((n_seq, n_rep)),
            dma((n_seq,)),
            dma((depth,)),
            dma((depth - 1,)),
        ],
        compiler_params=pltpu.CompilerParams(
            collective_id=1, has_side_effects=True, vmem_limit_bytes=VMEM_BUDGET
        ),
    )(order, q, k, v, wo, resid, gain, w_gate, w_up, w_down)


def kernels_fit(queries, wo, w_gate):
    n_seq, n_rep = lax.axis_size("seq"), lax.axis_size("rep")
    columns = wo.shape[1]
    sub = queries.shape[0] // (n_rep * lax.axis_size("section"))
    tokens = n_seq * sub
    half = w_gate.shape[0] // n_rep
    held = 3 * half * w_gate.shape[1] * 2 + n_seq * tokens * columns * 18 + 20 * tokens * half
    return (
        n_rep == 2
        and n_seq % 2 == 0
        and n_seq >= 4
        and columns % 128 == 0
        and tokens % 128 == 0
        and sub % 16 == 0
        and queries.shape[0] % (16 * PIECES) == 0
        and half % 16 == 0
        and held < VMEM_BUDGET - 8 * 2**20
    )


def on_device(queries, keys, values, block_order, wo, resid, gain, w_gate, w_up, w_down):
    seq_dev = queries.shape[0]
    heads_dev = queries.shape[1] // HEAD_DIM
    groups = lax.axis_size("section") * lax.axis_size("rep")
    n_seq = lax.axis_size("seq")
    sub_rows = seq_dev // groups
    block_rows = seq_dev // 2
    query_start = lax.axis_index("seq") * seq_dev
    query_pos = key_positions(block_order, query_start, seq_dev, block_rows)
    if kernels_fit(queries, wo, w_gate):
        block = resid.reshape(wo.shape[1], n_seq * sub_rows)
        mixed = layer(block_order, queries, keys, values, wo, block, gain, w_gate, w_up, w_down)
        return mixed.reshape(resid.shape)
    query_heads = queries.reshape(seq_dev, heads_dev, HEAD_DIM)
    scale = HEAD_DIM ** (-0.5)
    running_max = jnp.full((seq_dev, heads_dev), -1e30, jnp.float32)
    key_piece = lax.all_gather(keys, "seq", axis=0, tiled=True)
    value_piece = lax.all_gather(values, "seq", axis=0, tiled=True)
    count = key_piece.shape[0]
    key_pos = key_positions(block_order, jnp.int32(0), count, block_rows)
    scores = (
        jnp.einsum(
            "qhd,khd->qhk",
            query_heads,
            key_piece.reshape(count, heads_dev, HEAD_DIM),
            preferred_element_type=jnp.float32,
        )
        * scale
    )
    visible = (key_pos[None, :] <= query_pos[:, None])[:, None, :]
    new_max = jnp.maximum(running_max, jnp.max(jnp.where(visible, scores, -1e30), axis=-1))
    probs = jnp.where(visible, jnp.exp(scores - new_max[..., None]), 0.0)
    total = jnp.sum(probs, axis=-1)
    weighted = jnp.einsum(
        "qhk,khd->qhd",
        probs.astype(jnp.bfloat16),
        value_piece.reshape(count, heads_dev, HEAD_DIM),
        preferred_element_type=jnp.float32,
    )
    running_max, total, weighted = (new_max, total, weighted)
    attended = (
        (weighted / total[..., None]).astype(jnp.bfloat16).reshape(seq_dev, heads_dev * HEAD_DIM)
    )
    columns = wo.shape[1]
    token_count = n_seq * sub_rows
    parts = attended.reshape(groups, sub_rows, heads_dev * HEAD_DIM)
    group_rows = lax.all_to_all(parts, ("section", "rep"), split_axis=0, concat_axis=2, tiled=True)
    wo_columns = lax.all_gather(wo, ("section", "rep"), axis=0, tiled=True)
    piece = lax.all_gather(group_rows, "seq", axis=0, tiled=True)
    flat = piece.reshape(piece.shape[0] * piece.shape[1], piece.shape[2])
    product = jnp.dot(flat, wo_columns, preferred_element_type=jnp.float32)
    projected = product.reshape(piece.shape[0], piece.shape[1], columns)
    projected_cols = projected.reshape(token_count, columns).T
    carried = resid.reshape(columns, token_count).astype(jnp.float32) + projected_cols
    squares = lax.psum(jnp.sum(carried * carried, axis=0), "seq")
    normed = (
        carried * lax.rsqrt(squares / D + 1e-05)[None, :] * gain.astype(jnp.float32)[:, None]
    ).astype(jnp.bfloat16)
    piece = lax.all_gather(normed, "seq", axis=0, tiled=True)
    gate_sum = jnp.dot(w_gate, piece, preferred_element_type=jnp.float32)
    up_sum = jnp.dot(w_up, piece, preferred_element_type=jnp.float32)
    hidden = (jax.nn.silu(gate_sum) * up_sum).astype(jnp.bfloat16)
    term = lax.dot_general(
        w_down, hidden, (((0,), (0,)), ((), ())), preferred_element_type=jnp.float32
    )
    down = lax.psum_scatter(term, "seq", scatter_dimension=0, tiled=True)
    return (carried + down).astype(jnp.bfloat16).reshape(resid.shape)


def solution(mesh):
    return jax.shard_map(
        on_device,
        mesh=mesh,
        in_specs=(
            P("seq", ("section", "rep")),
            P("seq", ("section", "rep")),
            P("seq", ("section", "rep")),
            P(),
            P(("section", "rep"), "seq"),
            P(("section", "rep"), "seq", None),
            P("seq"),
            P("seq", None),
            P("seq", None),
            P("seq", None),
        ),
        out_specs=P(("section", "rep"), "seq", None),
        check_vma=False,
    )
```
